32 devices in a mesh: gz: 16 (over z, x, core), xy: 2 (over y).
Axes of the slice: x: 2, y: 2, z: 4, core: 2. Of those that a mesh axis runs over, the one named last changes fastest.
Arguments:
- coords: float32 [3, 32, 4, 128], P(None, 'gz', 'xy'), may hold values from 0 to 1
- species: int32 [32, 4, 128], P('gz', 'xy'), may hold values from 0 to 7
- centers: int32 [32, 4, 128], P('gz', 'xy'), may hold values from 0 to 127
- others: int32 [32, 4, 128], P('gz', 'xy'), may hold values from 0 to 1151
- live_count: int32 [32, 4], P('gz', 'xy'), may hold values from 42 to 128
- in_weight: float32 [24, 128], replicated, may hold values from -1.25 to 1.25
- env_weight: float32 [128, 32], replicated, may hold values from -0.5 to 0.5
- up_weight: float32 [160, 128], replicated, may hold values from -0.5 to 0.5
- out_weight: float32 [128], replicated, may hold values from -0.5 to 0.5
Outputs:
- atom_energy: float32 [32, 4, 128], P('gz', 'xy')
- forces: float32 [3, 32, 4, 128], P(None, 'gz', 'xy')
The draws below stay inside these ranges and needn't reach their ends.
Inputs may be any that keep to these rules, and one draw needn't show every extreme that they name: Edge slots at or after live_count of a bin are padding; at most 128 are live.
All inputs are finite; a program needn't handle non-finite values.
Results may differ from the reference program's by a relative error of at most 0.0018.
Values may be sent and summed in bfloat16 or wider, within the bound.
A program may use at most 64 MiB of HBM per device.

```python
import jax
import jax.numpy as jnp
from jax import lax

BIN = 128
NB = 8
SPEC = 8
LAT = 128
CH = 32
EDGES = 128
NBZ = 32
NBX = 4


def touch_ends(array, own_key, least, largest):
    longest = array.shape.index(max(array.shape))
    spots = []
    for shift in (0, 1):
        where = [jax.random.randint(jax.random.fold_in(own_key, axis), (), 0, length) for axis, length in enumerate(array.shape)]
        where[longest] = (where[longest] + shift) % array.shape[longest]
        spots.append(tuple(where))
    return array.at[spots[0]].set(least).at[spots[1]].set(largest)


def levels(rng, shape, cuts, smallest, high):
    gain, own = 1.0, jax.random.fold_in(rng, 6)
    for axis_at, shards_of in cuts:
        steps = jnp.exp(jax.random.uniform(jax.random.fold_in(own, axis_at), (shards_of,), jnp.float32, smallest / len(cuts), high / len(cuts)))
        gain = gain * jnp.repeat(steps, shape[axis_at] // shards_of).reshape([-1 if axis == axis_at else 1 for axis in range(len(shape))])
    return gain


def scatter_about(key, extent, spread, reach, kind=jnp.bfloat16):
    return jnp.clip(spread * jax.random.normal(key, extent, jnp.float32), -reach, reach).astype(kind)


def setup_inputs(seed: int = 0) -> dict:
    arg_keys = jax.random.split(jax.random.key(seed), 10)
    return {
        "coords": jnp.clip(1.0 * jax.random.uniform(arg_keys[0], (3, NBZ, NBX, BIN), jnp.float32) ** levels(arg_keys[0], (3, NBZ, NBX, BIN), ((1, 16), (2, 2)), -0.2, 0.2), 0.0, 1.0),
        "species": touch_ends(jax.random.randint(arg_keys[1], (NBZ, NBX, BIN), 0, SPEC), jax.random.fold_in(arg_keys[1], 1), 0, SPEC - 1).astype(jnp.int32),
        "centers": touch_ends(jax.random.randint(arg_keys[2], (NBZ, NBX, EDGES), 0, BIN), jax.random.fold_in(arg_keys[2], 1), 0, BIN - 1).astype(jnp.int32),
        "others": touch_ends(jax.random.randint(arg_keys[3], (NBZ, NBX, EDGES), 0, 9 * BIN), jax.random.fold_in(arg_keys[3], 1), 0, (9 * BIN) - 1).astype(jnp.int32),
        "live_count": touch_ends(jax.random.randint(arg_keys[4], (NBZ, NBX), EDGES // 3, EDGES + 1), jax.random.fold_in(arg_keys[4], 1), EDGES // 3, EDGES).astype(jnp.int32),
        "in_weight": scatter_about(arg_keys[5], (NB + 2 * SPEC, LAT), (NB + 2 * SPEC) ** -0.5, 1.25, jnp.float32),
        "env_weight": scatter_about(arg_keys[6], (LAT, CH), LAT ** -0.5, 0.5, jnp.float32),
        "up_weight": scatter_about(arg_keys[7], (LAT + CH, LAT), (LAT + CH) ** -0.5, 0.5, jnp.float32),
        "out_weight": scatter_about(arg_keys[8], (LAT,), LAT ** -0.5, 0.5, jnp.float32),
    }


SOFTEN = 0.01
CUTOFF = 3.5
HIGH = lax.Precision.HIGHEST

def neighbourhood(lattice):
    depth_bins = lattice.shape[-3] - 2
    span_bins = lattice.shape[-2] - 2
    blocks = []
    for offset in range(9):
        start_z = offset // 3
        start_x = offset % 3
        blocks.append(lattice[..., start_z:start_z + depth_bins, start_x:start_x + span_bins, :])
    return jnp.concatenate(blocks, axis=-1)

def pick(lattice, indices):
    return jnp.take_along_axis(lattice, jnp.broadcast_to(indices, lattice.shape[:1] + indices.shape), axis=-1)

def live_mask(live_count, edge_count):
    return (jnp.arange(edge_count)[None, None, :] < live_count[..., None]).astype(jnp.float32)

def geometry(coord_ext, spec_ext, centers, others, in_weight):
    interior = coord_ext[:, 1:-1, 1:-1]
    at_center = pick(interior, centers)
    at_other = pick(neighbourhood(coord_ext), others)
    placement = others // 128
    shift_z = (placement // 3 - 1).astype(jnp.float32)
    shift_x = (placement % 3 - 1).astype(jnp.float32)
    along_z = shift_z + at_other[0] - at_center[0]
    across = shift_x + at_other[1] - at_center[1]
    along_y = at_other[2] - at_center[2]
    distance = jnp.sqrt(along_z * along_z + across * across + along_y * along_y + SOFTEN)
    scaled = distance / CUTOFF
    envelope = (1.0 - scaled * scaled) ** 2
    orders = jnp.arange(1, NB + 1).astype(jnp.float32)[:, None, None, None]
    radial = jnp.sin(orders * jnp.pi * scaled[None]) / distance[None] * envelope[None]
    species_ids = jnp.arange(SPEC).astype(spec_ext.dtype)[:, None, None, None]
    spec_center = pick(spec_ext[None, 1:-1, 1:-1], centers)
    spec_other = pick(neighbourhood(spec_ext[None]), others)
    inputs = jnp.concatenate([radial, (spec_center == species_ids).astype(jnp.float32), (spec_other == species_ids).astype(jnp.float32)], axis=0)
    latent = jax.nn.silu(jnp.einsum('kabe,kl->labe', inputs, in_weight, precision=HIGH))
    harmonics = jnp.stack([jnp.ones_like(distance), along_z / distance, across / distance, along_y / distance])
    return (latent, harmonics, envelope)

def features(latent, harmonics, centers, live_count, env_weight):
    edge_count = centers.shape[-1]
    weights = jnp.einsum('labe,lc->cabe', latent, env_weight, precision=HIGH) * live_mask(live_count, edge_count)[None]
    messages = (weights[:, None] * harmonics[None]).reshape((-1,) + centers.shape)
    one_hot = (centers[..., None] == jnp.arange(128)).astype(jnp.float32)
    return jnp.einsum('fabe,aben->fabn', messages, one_hot, precision=HIGH) * (128.0 / edge_count)

def energy(latent, envelope, feature_ext, centers, others, live_count, up_weight, out_weight):
    channels = feature_ext.shape[0] // 4
    feat_center = pick(feature_ext[:, 1:-1, 1:-1], centers)
    feat_other = pick(neighbourhood(feature_ext), others)
    products = (feat_center * feat_other).reshape((channels, 4) + centers.shape).sum(axis=1)
    joined = jnp.concatenate([latent, products], axis=0)
    hidden = jax.nn.silu(jnp.einsum('kabe,kl->labe', joined, up_weight, precision=HIGH))
    edge_energy = jnp.einsum('labe,l->abe', hidden, out_weight, precision=HIGH) * envelope * live_mask(live_count, centers.shape[-1])
    one_hot = (centers[..., None] == jnp.arange(128)).astype(jnp.float32)
    atom_energy = jnp.einsum('abe,aben->abn', edge_energy, one_hot, precision=HIGH)
    return (jnp.sum(edge_energy), atom_energy)

def wrap_pad(lattice, first_dim):
    widths = [(0, 0)] * lattice.ndim
    widths[first_dim] = (1, 1)
    widths[first_dim + 1] = (1, 1)
    return jnp.pad(lattice, widths, mode='wrap')

def reference(coords, species, centers, others, live_count, in_weight, env_weight, up_weight, out_weight):
    row_count = coords.shape[1]
    spec_pad = wrap_pad(species, 0)
    row_ids = jnp.arange(row_count).astype(jnp.int32)

    def total(coords_now):
        coord_pad = wrap_pad(coords_now, 1)

        def row_latent(row_index):
            coord_block = lax.dynamic_slice_in_dim(coord_pad, row_index, 3, 1)
            spec_block = lax.dynamic_slice_in_dim(spec_pad, row_index, 3, 0)
            center_row = lax.dynamic_slice_in_dim(centers, row_index, 1, 0)
            other_row = lax.dynamic_slice_in_dim(others, row_index, 1, 0)
            live_row = lax.dynamic_slice_in_dim(live_count, row_index, 1, 0)
            return (geometry(coord_block, spec_block, center_row, other_row, in_weight), center_row, other_row, live_row)

        def feature_row(row_index):
            (latent, harmonics, envelope), center_row, other_row, live_row = row_latent(row_index)
            return features(latent, harmonics, center_row, live_row, env_weight)
        stacked = lax.map(jax.checkpoint(feature_row), row_ids)
        features_all = jnp.moveaxis(stacked[:, :, 0], 0, 1)
        rounded = lax.optimization_barrier(features_all.astype(jnp.bfloat16)).astype(jnp.float32)
        through = features_all + lax.stop_gradient(rounded - features_all)
        feature_pad = wrap_pad(through, 1)

        def energy_row(row_index):
            (latent, harmonics, envelope), center_row, other_row, live_row = row_latent(row_index)
            feature_block = lax.dynamic_slice_in_dim(feature_pad, row_index, 3, 1)
            return energy(latent, envelope, feature_block, center_row, other_row, live_row, up_weight, out_weight)
        row_sums, row_atoms = lax.map(jax.checkpoint(energy_row), row_ids)
        return (jnp.sum(row_sums), row_atoms[:, 0])
    (energy_total, atom_energy), gradient = jax.value_and_grad(total, has_aux=True)(coords)
    return (atom_energy, -gradient)
```

```python
import functools
import math

import jax
import jax.numpy as jnp
from jax import lax
from jax.experimental import pallas as pl
from jax.experimental.pallas import tpu as pltpu
from jax.sharding import PartitionSpec as P

SOFTEN = 0.01
CUTOFF = 3.5
F32 = jnp.float32
BF16 = jnp.bfloat16
MESH = pl.DeviceIdType.MESH


def rounded(x):
    return x.astype(BF16).astype(F32)


def split(x):
    high = x.astype(BF16)
    return high, (x - high.astype(F32)).astype(BF16)


def dot(a, b):
    return jnp.dot(a, b, preferred_element_type=F32)


def dot_t(a, b):
    return lax.dot_general(a, b, (((1,), (1,)), ((), ())), preferred_element_type=F32)


def join(parts, axis):
    return parts[0] if len(parts) == 1 else jnp.concatenate(parts, axis=axis)


def neighbours(nz, nx):
    slots = {(0, 0): 0}
    for dz in (-1, 0, 1):
        for dx in (-1, 0, 1):
            slots.setdefault((dz % nz, dx % nx), len(slots))
    return slots


def kernel(
    nz, nx, bz, bx, nb, spec, ch, lat,
    coords_hbm, species_hbm, centers_hbm, others_hbm, live_hbm, in_hbm, env_hbm, up_hbm, out_hbm,
    result_ref,
    coords_ref, species_ref, centers_ref, others_ref, live_ref, in_ref, env_ref, up_ref, out_ref,
    halo, tab, ct, ot, rows_live, rows_p, geo, xs, sins, coss, rad, harm,
    l2, dsilu, wts, feat, dfeat, dlat_own, env_grad, dharm, drad, gr, grad, back,
    send1, recv1, send2, recv2, load_sem,
):
    n = coords_ref.shape[-1]
    slots = neighbours(nz, nx)
    me_z, me_x = lax.axis_index("gz"), lax.axis_index("xy")
    mine = slots[(1 % nz, 0)]
    others_list = [(key, s) for key, s in slots.items() if s != mine]
    index = {s: i for i, (_, s) in enumerate(others_list)}

    def owner(key):
        return (lax.rem(me_z + (key[0] - 1) % nz, nz), lax.rem(me_x + key[1], nx))

    def user(key):
        return (lax.rem(me_z + (1 - key[0]) % nz, nz), lax.rem(me_x + (-key[1]) % nx, nx))

    barrier = pltpu.get_barrier_semaphore()
    for key, _ in others_list:
        pl.semaphore_signal(barrier, inc=1, device_id=owner(key), device_id_type=MESH)

    loads = [
        pltpu.make_async_copy(source, target, load_sem.at[k])
        for k, (source, target) in enumerate([
            (coords_hbm, coords_ref), (species_hbm, species_ref), (centers_hbm, centers_ref),
            (others_hbm, others_ref), (live_hbm, live_ref), (in_hbm, in_ref), (env_hbm, env_ref),
            (up_hbm, up_ref), (out_hbm, out_ref)])
    ]
    for load in loads:
        load.start()
    for load in loads[:5]:
        load.wait()
    lane = lax.broadcasted_iota(jnp.int32, (1, n), 1)
    for a in range(bz):
        for b in range(bx):
            alive = (lane < live_ref[a : a + 1, b : b + 1]).astype(F32)
            halo[mine, a, b] = jnp.concatenate(
                [
                    coords_ref[:, a, b, :],
                    species_ref[a, b : b + 1, :].astype(F32),
                    centers_ref[a, b : b + 1, :].astype(F32),
                    others_ref[a, b : b + 1, :].astype(F32),
                    alive,
                    jnp.zeros((1, n), F32),
                ],
                axis=0,
            )
    pl.semaphore_wait(barrier, len(others_list))
    first = []
    for key, s in others_list:
        i = index[s]
        copy = pltpu.make_async_remote_copy(
            src_ref=halo.at[mine], dst_ref=halo.at[s], send_sem=send1.at[i],
            recv_sem=recv1.at[i], device_id=user(key), device_id_type=MESH,
        )
        copy.start()
        first.append(copy)

    for load in loads[5:]:
        load.wait()
    w_in = in_ref[...]
    w_hi = rounded(w_in)
    w_lo = w_in - w_hi
    w_rows = jnp.concatenate(
        [w_hi[:nb], w_lo[:nb], w_hi[:nb], w_hi[nb:], w_lo[nb:],
         jnp.zeros((lat - 3 * nb - 4 * spec, lat), F32)], axis=0)
    kin = (3 * nb + 4 * spec + 15) // 16 * 16
    in_t = w_rows.T.astype(BF16)[:, :kin]
    pad8 = jnp.zeros((nb, lat), F32)
    wr_hi = jnp.concatenate([w_hi[:nb], pad8], axis=0).astype(BF16)
    wr_lo = jnp.concatenate([w_lo[:nb], pad8], axis=0).astype(BF16)
    wr3 = jnp.concatenate([wr_hi, wr_hi, wr_lo], axis=1)
    env_t = env_ref[...]
    et_hi = rounded(env_t)
    et_lo = env_t - et_hi
    env_t3 = jnp.concatenate([et_hi, et_hi, et_lo], axis=1).astype(BF16)
    kpad = -(3 * ch) % lat
    env3 = jnp.concatenate(
        [et_hi, et_hi, et_lo] + ([jnp.zeros((kpad, lat), F32)] if kpad else []), axis=0
    ).T.astype(BF16)
    up = up_ref[...]
    up_hi = rounded(up)
    up_lo = up - up_hi
    up3 = jnp.concatenate([up_hi, up_hi, up_lo], axis=1).astype(BF16)
    up_t = jnp.concatenate(
        [x.T.astype(BF16) for x in (up_hi[:lat], up_hi[:lat], up_lo[:lat])]
        + [jnp.concatenate(
            [up_hi[lat:], up_hi[lat:], up_lo[lat:]]
            + ([jnp.zeros((kpad, lat), F32)] if kpad else []), axis=0).T.astype(BF16)],
        axis=1)
    out_col = jnp.broadcast_to(out_ref[...], (n, lat)).T

    cells = [(a, b) for a in range(bz - 1, 2 * bz + 1) for b in range(bx - 1, 2 * bx + 1)]
    row_n = lax.broadcasted_iota(jnp.int32, (n, n), 0)

    def hots_of(i, part):
        o = part[5:6].astype(jnp.int32)
        ct[i] = (row_n == part[4:5].astype(jnp.int32)).astype(F32).astype(BF16)
        ot[i] = (row_n == (o & 127)).astype(F32).astype(BF16)

    for copy in first:
        copy.wait()

    def place(a, b):
        return slots[((a // bz - 1) % nz, (b // bx - 1) % nx)], a % bz, b % bx

    def block(a, b):
        s, i, j = place(a, b)
        return halo[s, i, j]

    window_z = range(bz - 2, 2 * bz + 2)
    window_x = range(bx - 2, 2 * bx + 2)
    for a in window_z:
        for b in window_x:
            part = block(a, b)
            hi = rounded(part)
            tab[a, b] = jnp.concatenate([hi, part - hi], axis=0).astype(BF16)

    cx = bx + 2
    total = len(cells)
    row_s = lax.broadcasted_iota(jnp.int32, (spec, n), 0).astype(F32)
    for i, (a, b) in enumerate(cells):
        part = block(a, b)
        o = part[5:6].astype(jnp.int32)
        p = o >> 7
        hots_of(i, part)
        hot_c, hot_o = ct[i], ot[i]
        at_c = dot(tab[a, b], hot_c)
        at_c = at_c[:8] + at_c[8:]
        around = jnp.concatenate(
            [tab[a + dz, b + dx] for dz in (-1, 0, 1) for dx in (-1, 0, 1)], axis=0)
        got = dot(around, hot_o)
        at_o = jnp.zeros((8, n), F32)
        for off in range(9):
            at_o = jnp.where(p == off, got[16 * off : 16 * off + 8] + got[16 * off + 8 : 16 * off + 16], at_o)
        diff = at_o - at_c
        up3_ = (p >= 3).astype(jnp.int32) + (p >= 6).astype(jnp.int32)
        geo[0, i : i + 1] = diff[0:1] + (up3_ - 1).astype(F32)
        geo[1, i : i + 1] = diff[1:2] + (p - 3 * up3_ - 1).astype(F32)
        geo[2, i : i + 1] = diff[2:3]
        xs[:spec, i * n : (i + 1) * n] = (row_s == at_c[3:4]).astype(F32)
        xs[spec:, i * n : (i + 1) * n] = (row_s == at_o[3:4]).astype(F32)
        rows_live[i : i + 1] = part[6:7]
        rows_p[i : i + 1] = p

    r = [geo[m] for m in range(3)]
    dist = jnp.sqrt(r[0] * r[0] + r[1] * r[1] + r[2] * r[2] + SOFTEN)
    inv = 1.0 / dist
    q = dist / CUTOFF
    rest = 1.0 - q * q
    envelope = rest * rest
    scale = inv * envelope
    s1 = jnp.sin(math.pi * q)
    c1 = jnp.cos(math.pi * q)
    s0, c0, sk, ck = jnp.zeros_like(s1), jnp.ones_like(c1), s1, c1
    for k in range(nb):
        sins[k] = sk
        coss[k] = ck
        rad[k] = sk * scale
        s0, sk = sk, 2.0 * c1 * sk - s0
        c0, ck = ck, 2.0 * c1 * ck - c0
    for m in range(3):
        harm[m] = r[m] * inv
    env_grad[...] = jnp.zeros_like(env_grad)
    geo[3] = envelope

    interior = {}
    for i, (a, b) in enumerate(cells):
        if bz <= a < 2 * bz and bx <= b < 2 * bx:
            interior[i] = (a - bz) * bx + (b - bx)

    group = 4 if total % 4 == 0 else 1
    for g in range(0, total, group):
        ids = list(range(g, g + group))
        span = slice(g * n, (g + group) * n)
        radial = join([rad[:, i, :] for i in ids], 1)
        rh = rounded(radial)
        x_s = xs[:, span]
        parts = [rh, rh, radial - rh, x_s, x_s]
        fill = kin - 3 * nb - 4 * spec
        if fill:
            parts.append(jnp.zeros((fill, group * n), F32))
        pre = dot(in_t, jnp.concatenate(parts, axis=0).astype(BF16))
        sig = 1.0 / (1.0 + jnp.exp(-pre))
        latent = pre * sig
        dsilu[:, span] = sig + latent * (1.0 - sig)
        lh, ll = split(latent)
        for t, i in enumerate(ids):
            if i in interior:
                l2[interior[i], 0] = lh[:, t * n : (t + 1) * n]
                l2[interior[i], 1] = ll[:, t * n : (t + 1) * n]
        alive = join([rows_live[i : i + 1] for i in ids], 1)
        w = dot(env_t3, jnp.concatenate([lh, ll, lh], axis=0)) * alive
        wts[:, span] = w
        msgs = jnp.concatenate(
            [w] + [w * join([harm[m, i : i + 1] for i in ids], 1) for m in range(3)], axis=0)
        mh, ml = split(msgs)
        for t, i in enumerate(ids):
            cut = slice(t * n, (t + 1) * n)
            hot_c = ct[i]
            feat[:, i * n : (i + 1) * n] = dot_t(
                jnp.concatenate([mh[:, cut], ml[:, cut]], axis=1),
                jnp.concatenate([hot_c, hot_c], axis=1)).astype(BF16)

    dfeat[...] = jnp.zeros_like(dfeat)
    grad[...] = jnp.zeros_like(grad)
    row_8 = lax.broadcasted_iota(jnp.int32, (16, n), 0)
    for i, k in interior.items():
        hot_c, hot_o = ct[i], ot[i]
        p = rows_p[i : i + 1]
        env_row = geo[3, i : i + 1]
        alive = rows_live[i : i + 1]
        f_c = dot(feat[:, i * n : (i + 1) * n], hot_c)
        f_o = None
        hots = []
        for dz in range(3):
            start = i + (dz - 1) * cx - 1
            hot3 = jnp.concatenate(
                [hot_o * (p == 3 * dz + dx).astype(F32).astype(BF16) for dx in range(3)], axis=0)
            hots.append((start, hot3))
            term = dot(feat[:, start * n : (start + 3) * n], hot3)
            f_o = term if f_o is None else f_o + term
        prod4 = f_c * f_o
        prod = prod4[:ch] + prod4[ch : 2 * ch] + prod4[2 * ch : 3 * ch] + prod4[3 * ch :]
        ph, pl_ = split(prod)
        parts = [l2[k, 0], l2[k, 1], l2[k, 0], ph, pl_, ph]
        if kpad:
            parts.append(jnp.zeros((kpad, n), BF16))
        u = dot(up_t, jnp.concatenate(parts, axis=0))
        sig = 1.0 / (1.0 + jnp.exp(-u))
        hid = u * sig
        raw = jnp.sum(out_col * hid, axis=0, keepdims=True) * alive
        env_grad[i : i + 1] = raw
        e_row = raw * env_row
        e_hi = rounded(e_row)
        e_rows = jnp.where(row_8 == 0, e_hi, jnp.where(row_8 == 1, e_row - e_hi, 0.0)).astype(BF16)
        e_atom = dot_t(e_rows, hot_c)
        grad[0, k // bx, k % bx, 3:4] = -(e_atom[0:1] + e_atom[1:2])
        d_u = out_col * (alive * env_row) * (sig + hid * (1.0 - sig))
        dh, dl = split(d_u)
        d_join = dot(up3, jnp.concatenate([dh, dl, dh], axis=0))
        dlat_own[k] = d_join[:lat]
        d_prod = jnp.concatenate([d_join[lat:]] * 4, axis=0)
        dch, dcl = split(d_prod * f_o)
        doh, dol = split(d_prod * f_c)
        dfeat[:, i * n : (i + 1) * n] += dot_t(
            jnp.concatenate([dch, dcl], axis=1), jnp.concatenate([hot_c, hot_c], axis=1))
        d_o = jnp.concatenate([doh, dol], axis=1)
        for start, hot3 in hots:
            dfeat[:, start * n : (start + 3) * n] += dot_t(
                d_o, jnp.concatenate([hot3, hot3], axis=1))

    for g in range(0, total, group):
        ids = list(range(g, g + group))
        span = slice(g * n, (g + group) * n)
        dm = []
        for i in ids:
            hot_c = ct[i]
            fh, fl = split(dfeat[:, i * n : (i + 1) * n])
            dm.append(dot(jnp.concatenate([fh, fl], axis=1), jnp.concatenate([hot_c, hot_c], axis=0)))
        dm = join(dm, 1)
        w = wts[:, span]
        dw = dm[:ch]
        for m in range(3):
            piece = dm[(m + 1) * ch : (m + 2) * ch]
            dw = dw + piece * join([harm[m, i : i + 1] for i in ids], 1)
            d_h = jnp.sum(piece * w, axis=0, keepdims=True)
            for t, i in enumerate(ids):
                dharm[m, i : i + 1] = d_h[:, t * n : (t + 1) * n]
        dw = dw * join([rows_live[i : i + 1] for i in ids], 1)
        wh, wl = split(dw)
        parts = [wh, wl, wh]
        if kpad:
            parts.append(jnp.zeros((kpad, group * n), BF16))
        d_lat = dot(env3, jnp.concatenate(parts, axis=0))
        if any(i in interior for i in ids):
            d_lat = d_lat + join(
                [dlat_own[interior[i]] if i in interior else jnp.zeros((lat, n), F32) for i in ids], 1)
        dh, dl = split(d_lat * dsilu[:, span])
        d_r = dot(wr3, jnp.concatenate([dh, dl, dh], axis=0))
        for t, i in enumerate(ids):
            drad[:, i, :] = d_r[:nb, t * n : (t + 1) * n]

    sum_s = drad[0] * sins[0]
    sum_c = drad[0] * coss[0]
    for k in range(1, nb):
        sum_s = sum_s + drad[k] * sins[k]
        sum_c = sum_c + (k + 1.0) * (drad[k] * coss[k])
    env_slope = (-4.0 / CUTOFF) * q * rest
    d_dist = (
        (math.pi / CUTOFF) * sum_c * scale
        - sum_s * scale * inv
        + (sum_s * inv + env_grad[...]) * env_slope
    )
    for m in range(3):
        d_dist = d_dist - dharm[m] * r[m] * (inv * inv)
    gr[...] = jnp.zeros_like(gr)
    for m in range(3):
        d_m = d_dist * harm[m] + dharm[m] * inv
        hi = rounded(d_m)
        gr[:, m, :] = hi
        gr[:, m + 4, :] = d_m - hi

    second = {}

    def give(ready):
        for key, s in others_list:
            if s in second or not ready(s):
                continue
            i = index[s]
            second[s] = pltpu.make_async_remote_copy(
                src_ref=grad.at[s], dst_ref=back.at[i], send_sem=send2.at[i],
                recv_sem=recv2.at[i], device_id=owner(key), device_id_type=MESH,
            )
            second[s].start()

    order = sorted(range(total), key=lambda i: (-cells[i][0], cells[i][1]))
    targets = [
        {place(cells[i][0] + dz, cells[i][1] + dx)[0] for dz in (-1, 0, 1) for dx in (-1, 0, 1)}
        for i in order]
    for turn, i in enumerate(order):
        a, b = cells[i]
        g8 = gr[i]
        p = rows_p[i : i + 1]
        at_c = dot_t(jnp.concatenate([g8, jnp.zeros_like(g8)], axis=0).astype(BF16), ct[i])
        stack = [jnp.where(p == off, g8, 0.0) for off in range(9)] + [jnp.zeros_like(g8)]
        at_o = dot_t(jnp.concatenate(stack, axis=0).astype(BF16), ot[i])
        s, y, x = place(a, b)
        grad[s, y, x] -= at_c[:8]
        for off in range(9):
            s, y, x = place(a + off // 3 - 1, b + off % 3 - 1)
            grad[s, y, x] += at_o[8 * off : 8 * off + 8]
        if turn + 1 < total and b == cells[-1][1]:
            later = set().union(*targets[turn + 1 :])
            give(lambda s: s not in later)
    give(lambda s: True)
    for copy in second.values():
        copy.wait()
    for a in range(bz):
        for b in range(bx):
            acc = grad[mine, a, b]
            for s in range(len(others_list)):
                acc = acc + back[s, a, b]
            result_ref[:, a, b, :] = -(acc[:4] + acc[4:])


def solution(mesh):
    nz, nx = mesh.shape["gz"], mesh.shape["xy"]

    def body(coords, species, centers, others, live_count, in_weight, env_weight, up_weight, out_weight):
        _, bz, bx, n = coords.shape
        lat, ch = env_weight.shape
        nb = 8
        spec = (in_weight.shape[0] - nb) // 2
        cells = (bz + 2) * (bx + 2)
        ns = len(neighbours(nz, nx)) - 1
        vmem = lambda shape, dtype=F32: pltpu.VMEM(shape, dtype)
        args = (coords, species, centers, others, live_count, in_weight, env_weight.T, up_weight,
                out_weight[None])
        scratch = [vmem(x.shape, x.dtype) for x in args] + [
            vmem((ns + 1, bz, bx, 8, n)),
            vmem((3 * bz, 3 * bx, 16, n), BF16),
            vmem((cells, n, n), BF16),
            vmem((cells, n, n), BF16),
            vmem((cells, n)),
            vmem((cells, n), jnp.int32),
            vmem((4, cells, n)),
            vmem((2 * spec, cells * n)),
            vmem((nb, cells, n)),
            vmem((nb, cells, n)),
            vmem((nb, cells, n)),
            vmem((3, cells, n)),
            vmem((bz * bx, 2, lat, n), BF16),
            vmem((lat, cells * n)),
            vmem((ch, cells * n)),
            vmem((4 * ch, cells * n), BF16),
            vmem((4 * ch, cells * n)),
            vmem((bz * bx, lat, n)),
            vmem((cells, n)),
            vmem((3, cells, n)),
            vmem((nb, cells, n)),
            vmem((cells, 8, n)),
            vmem((ns + 1, bz, bx, 8, n)),
            vmem((ns, bz, bx, 8, n)),
        ] + [pltpu.SemaphoreType.DMA((ns,)) for _ in range(4)]
        scratch.append(pltpu.SemaphoreType.DMA((len(args),)))
        specs = [pl.BlockSpec(memory_space=pl.ANY) for _ in args]
        result = pl.pallas_call(
            functools.partial(kernel, nz, nx, bz, bx, nb, spec, ch, lat),
            out_shape=pltpu.VMEM((4, bz, bx, n), F32),
            in_specs=specs,
            out_specs=pl.BlockSpec(memory_space=pltpu.VMEM),
            scratch_shapes=scratch,
            compiler_params=pltpu.CompilerParams(collective_id=0, has_side_effects=True),
        )(*args)
        return result[3], result[:3]

    in_specs = (
        P(None, "gz", "xy", None), P("gz", "xy", None), P("gz", "xy", None), P("gz", "xy", None),
        P("gz", "xy"), P(), P(), P(), P(),
    )
    out_specs = (P("gz", "xy", None), P(None, "gz", "xy", None))
    return jax.shard_map(body, mesh=mesh, in_specs=in_specs, out_specs=out_specs, check_vma=False)
```

```python
import functools
import math

import jax
import jax.numpy as jnp
from jax import lax
from jax.experimental import pallas as pl
from jax.experimental.pallas import tpu as pltpu
from jax.sharding import PartitionSpec as P

SOFTEN = 0.01
CUTOFF = 3.5
F32 = jnp.float32
BF16 = jnp.bfloat16
MESH = pl.DeviceIdType.MESH


def rounded(x):
    return x.astype(BF16).astype(F32)


def split(x):
    high = x.astype(BF16)
    return high, (x - high.astype(F32)).astype(BF16)


def dot(a, b):
    return jnp.dot(a, b, preferred_element_type=F32)


def dot_t(a, b):
    return lax.dot_general(a, b, (((1,), (1,)), ((), ())), preferred_element_type=F32)


def join(parts, axis):
    return parts[0] if len(parts) == 1 else jnp.concatenate(parts, axis=axis)


def neighbours(nz, nx):
    slots = {(0, 0): 0}
    for dz in (-1, 0, 1):
        for dx in (-1, 0, 1):
            slots.setdefault((dz % nz, dx % nx), len(slots))
    return slots


def kernel(
    nz, nx, bz, bx, nb, spec, ch, lat,
    coords_hbm, species_hbm, centers_hbm, others_hbm, live_hbm, in_hbm, env_hbm, up_hbm, out_hbm,
    result_ref,
    coords_ref, species_ref, centers_ref, others_ref, live_ref, in_ref, env_ref, up_ref, out_ref,
    halo, tab, ct, ot, hot_rows, rows_live, rows_p, geo, xs, sins, coss, rad, harm,
    l2, dsilu, wts, feat, dfeat, dlat_own, env_grad, dharm, drad, gr, grad, back,
    send1, recv1, send2, recv2, load_sem,
):
    n = coords_ref.shape[-1]
    slots = neighbours(nz, nx)
    me_z, me_x = lax.axis_index("gz"), lax.axis_index("xy")
    mine = slots[(1 % nz, 0)]
    others_list = [(key, s) for key, s in slots.items() if s != mine]
    index = {s: i for i, (_, s) in enumerate(others_list)}

    def owner(key):
        return (lax.rem(me_z + (key[0] - 1) % nz, nz), lax.rem(me_x + key[1], nx))

    def user(key):
        return (lax.rem(me_z + (1 - key[0]) % nz, nz), lax.rem(me_x + (-key[1]) % nx, nx))

    barrier = pltpu.get_barrier_semaphore()
    for key, _ in others_list:
        pl.semaphore_signal(barrier, inc=1, device_id=owner(key), device_id_type=MESH)

    loads = [
        pltpu.make_async_copy(source, target, load_sem.at[k])
        for k, (source, target) in enumerate([
            (coords_hbm, coords_ref), (species_hbm, species_ref), (centers_hbm, centers_ref),
            (others_hbm, others_ref), (live_hbm, live_ref), (in_hbm, in_ref), (env_hbm, env_ref),
            (up_hbm, up_ref), (out_hbm, out_ref)])
    ]
    for load in loads:
        load.start()
    for load in loads[:5]:
        load.wait()
    lane = lax.broadcasted_iota(jnp.int32, (1, n), 1)
    for a in range(bz):
        for b in range(bx):
            alive = (lane < live_ref[a : a + 1, b : b + 1]).astype(F32)
            halo[mine, a, b] = jnp.concatenate(
                [
                    coords_ref[:, a, b, :],
                    species_ref[a, b : b + 1, :].astype(F32),
                    centers_ref[a, b : b + 1, :].astype(F32),
                    others_ref[a, b : b + 1, :].astype(F32),
                    alive,
                    jnp.zeros((1, n), F32),
                ],
                axis=0,
            )
    pl.semaphore_wait(barrier, len(others_list))
    first = []
    for key, s in others_list:
        i = index[s]
        copy = pltpu.make_async_remote_copy(
            src_ref=halo.at[mine], dst_ref=halo.at[s], send_sem=send1.at[i],
            recv_sem=recv1.at[i], device_id=user(key), device_id_type=MESH,
        )
        copy.start()
        first.append(copy)

    for load in loads[5:]:
        load.wait()
    w_in = in_ref[...]
    w_hi = rounded(w_in)
    w_lo = w_in - w_hi
    w_rows = jnp.concatenate(
        [w_hi[:nb], w_lo[:nb], w_hi[:nb], w_hi[nb:], w_lo[nb:],
         jnp.zeros((lat - 3 * nb - 4 * spec, lat), F32)], axis=0)
    kin = (3 * nb + 4 * spec + 15) // 16 * 16
    in_t = w_rows.T.astype(BF16)[:, :kin]
    pad8 = jnp.zeros((nb, lat), F32)
    wr_hi = jnp.concatenate([w_hi[:nb], pad8], axis=0).astype(BF16)
    wr_lo = jnp.concatenate([w_lo[:nb], pad8], axis=0).astype(BF16)
    wr3 = jnp.concatenate([wr_hi, wr_hi, wr_lo], axis=1)
    env_t = env_ref[...]
    et_hi = rounded(env_t)
    et_lo = env_t - et_hi
    env_t3 = jnp.concatenate([et_hi, et_hi, et_lo], axis=1).astype(BF16)
    kpad = -(3 * ch) % lat
    env3 = jnp.concatenate(
        [et_hi, et_hi, et_lo] + ([jnp.zeros((kpad, lat), F32)] if kpad else []), axis=0
    ).T.astype(BF16)
    up = up_ref[...]
    up_hi = rounded(up)
    up_lo = up - up_hi
    up3 = jnp.concatenate([up_hi, up_hi, up_lo], axis=1).astype(BF16)
    up_t = jnp.concatenate(
        [x.T.astype(BF16) for x in (up_hi[:lat], up_hi[:lat], up_lo[:lat])]
        + [jnp.concatenate(
            [up_hi[lat:], up_hi[lat:], up_lo[lat:]]
            + ([jnp.zeros((kpad, lat), F32)] if kpad else []), axis=0).T.astype(BF16)],
        axis=1)
    out_col = jnp.broadcast_to(out_ref[...], (n, lat)).T

    hot_rows[...] = jnp.zeros_like(hot_rows)
    grad[...] = jnp.zeros_like(grad)
    cz, cx = bz + 2, bx + 2
    total = cz * cx
    wide = cx * n
    inner = bx * n
    cells = [(a, b) for a in range(bz - 1, 2 * bz + 1) for b in range(bx - 1, 2 * bx + 1)]
    row_n = lax.broadcasted_iota(jnp.int32, (n, n), 0).astype(F32).astype(BF16)
    row_s = lax.broadcasted_iota(jnp.int32, (spec, n), 0).astype(F32)
    one, zero = jnp.ones((n, n), BF16), jnp.zeros((n, n), BF16)

    def place(a, b):
        return slots[((a // bz - 1) % nz, (b // bx - 1) % nx)], a % bz, b % bx

    def block(a, b):
        s, i, j = place(a, b)
        return halo[s, i, j]

    def tables(rows):
        for a in rows:
            for b in range(bx - 2, 2 * bx + 2):
                part = block(a, b)
                hi = rounded(part)
                tab[a, b] = jnp.concatenate([hi, part - hi], axis=0).astype(BF16)

    def gather(i):
        a, b = cells[i]
        part = block(a, b)
        o = part[5:6].astype(jnp.int32)
        p = o >> 7
        hot_c = jnp.where(row_n == part[4:5].astype(BF16), one, zero)
        hot_o = jnp.where(row_n == (o & 127).astype(F32).astype(BF16), one, zero)
        ct[i] = hot_c
        ot[i] = hot_o
        zr, xc = i // cx, i % cx
        if 1 <= zr <= bz and 1 <= xc <= bx:
            for dz in range(3):
                for dx in range(3):
                    col = xc - 1 + dx
                    hot_rows[zr - 1, (dz * cx + col) * n : (dz * cx + col + 1) * n, (xc - 1) * n : xc * n] = (
                        hot_o * (p == 3 * dz + dx).astype(F32).astype(BF16))
        at_c = dot(tab[a, b], hot_c)
        at_c = at_c[:8] + at_c[8:]
        around = jnp.concatenate(
            [tab[a + dz, b + dx] for dz in (-1, 0, 1) for dx in (-1, 0, 1)], axis=0)
        got = dot(around, hot_o)
        at_o = jnp.zeros((8, n), F32)
        for off in range(9):
            at_o = jnp.where(p == off, got[16 * off : 16 * off + 8] + got[16 * off + 8 : 16 * off + 16], at_o)
        diff = at_o - at_c
        up3_ = (p >= 3).astype(jnp.int32) + (p >= 6).astype(jnp.int32)
        geo[0, i : i + 1] = diff[0:1] + (up3_ - 1).astype(F32)
        geo[1, i : i + 1] = diff[1:2] + (p - 3 * up3_ - 1).astype(F32)
        geo[2, i : i + 1] = diff[2:3]
        xs[:spec, i * n : (i + 1) * n] = (row_s == at_c[3:4]).astype(F32)
        xs[spec:, i * n : (i + 1) * n] = (row_s == at_o[3:4]).astype(F32)
        rows_live[i : i + 1] = part[6:7]
        rows_p[i : i + 1] = p

    def geometry(c):
        r = [geo[m, c] for m in range(3)]
        dist = jnp.sqrt(r[0] * r[0] + r[1] * r[1] + r[2] * r[2] + SOFTEN)
        inv = 1.0 / dist
        q = dist / CUTOFF
        rest = 1.0 - q * q
        envelope = rest * rest
        scale = inv * envelope
        s1 = jnp.sin(math.pi * q)
        c1 = jnp.cos(math.pi * q)
        s0, c0, sk, ck = jnp.zeros_like(s1), jnp.ones_like(c1), s1, c1
        for k in range(nb):
            sins[k, c] = sk
            coss[k, c] = ck
            rad[k, c] = sk * scale
            s0, sk = sk, 2.0 * c1 * sk - s0
            c0, ck = ck, 2.0 * c1 * ck - c0
        for m in range(3):
            harm[m, c] = r[m] * inv
        env_grad[c] = jnp.zeros_like(q)
        geo[3, c] = envelope
        geo[4, c] = inv
        geo[5, c] = (-4.0 / CUTOFF) * q * rest

    def latents(rows):
        state = {}
        for zr in rows:
            ids = list(range(zr * cx, (zr + 1) * cx))
            span = slice(zr * wide, (zr + 1) * wide)
            radial = join([rad[:, i, :] for i in ids], 1)
            rh = rounded(radial)
            x_s = xs[:, span]
            parts = [rh, rh, radial - rh, x_s, x_s]
            fill = kin - 3 * nb - 4 * spec
            if fill:
                parts.append(jnp.zeros((fill, wide), F32))
            pre = dot(in_t, jnp.concatenate(parts, axis=0).astype(BF16))
            sig = 0.5 + 0.5 * jnp.tanh(0.5 * pre)
            latent = pre * sig
            dsilu[:, span] = sig + latent * (1.0 - sig)
            lh, ll = split(latent)
            if 1 <= zr <= bz:
                l2[zr - 1, 0] = lh[:, n : n + inner]
                l2[zr - 1, 1] = ll[:, n : n + inner]
            alive = join([rows_live[i : i + 1] for i in ids], 1)
            w = dot(env_t3, jnp.concatenate([lh, ll, lh], axis=0)) * alive
            wts[:, span] = w
            msgs = jnp.concatenate(
                [w] + [w * join([harm[m, i : i + 1] for i in ids], 1) for m in range(3)], axis=0)
            mh, ml = split(msgs)
            for t, i in enumerate(ids):
                cut = slice(t * n, (t + 1) * n)
                hot_c = ct[i]
                feat[:, i * n : (i + 1) * n] = dot_t(
                    jnp.concatenate([mh[:, cut], ml[:, cut]], axis=1),
                    jnp.concatenate([hot_c, hot_c], axis=1)).astype(BF16)

    early = [zr for zr in range(cz) if zr >= 2]
    late = [zr for zr in range(cz) if zr < 2]

    for copy, key in zip(first, [key for key, _ in others_list]):
        if key[0] != (-1) % nz:
            copy.wait()
    tables(range(bz, 2 * bz + 2))
    for i in range(2 * cx, cz * cx):
        gather(i)
    geometry(slice(2 * cx, cz * cx))
    latents(early)
    for copy, key in zip(first, [key for key, _ in others_list]):
        if key[0] == (-1) % nz:
            copy.wait()
    tables(range(bz - 2, bz))
    for i in range(2 * cx):
        gather(i)
    geometry(slice(0, 2 * cx))
    latents(late)

    row_8 = lax.broadcasted_iota(jnp.int32, (16, n), 0)
    out_rows = jnp.concatenate([out_col] * bx, axis=1)
    inner_rows = range(1, bz + 1)

    def ids_of(zr):
        return [zr * cx + b for b in range(1, bx + 1)]

    f_cs, f_os = {}, {}
    for zr in inner_rows:
        f_cs[zr] = join([dot(feat[:, i * n : (i + 1) * n], ct[i]) for i in ids_of(zr)], 1)
        f_os[zr] = dot(feat[:, (zr - 1) * wide : (zr + 2) * wide], hot_rows[zr - 1])
    us = {}
    for zr in inner_rows:
        prod4 = f_cs[zr] * f_os[zr]
        prod = prod4[:ch] + prod4[ch : 2 * ch] + prod4[2 * ch : 3 * ch] + prod4[3 * ch :]
        ph, pl_ = split(prod)
        parts = [l2[zr - 1, 0], l2[zr - 1, 1], l2[zr - 1, 0], ph, pl_, ph]
        if kpad:
            parts.append(jnp.zeros((kpad, inner), BF16))
        us[zr] = dot(up_t, jnp.concatenate(parts, axis=0))
    joins, raws = {}, {}
    for zr in inner_rows:
        env_row = join([geo[3, i : i + 1] for i in ids_of(zr)], 1)
        alive = join([rows_live[i : i + 1] for i in ids_of(zr)], 1)
        u = us[zr]
        sig = 0.5 + 0.5 * jnp.tanh(0.5 * u)
        hid = u * sig
        raws[zr] = jnp.sum(out_rows * hid, axis=0, keepdims=True) * alive
        d_u = out_rows * (alive * env_row) * (sig + hid * (1.0 - sig))
        dh, dl = split(d_u)
        joins[zr] = dot(up3, jnp.concatenate([dh, dl, dh], axis=0))
    for zr in inner_rows:
        d_join = joins[zr]
        dlat_own[zr - 1] = d_join[:lat]
        d_prod = jnp.concatenate([d_join[lat:]] * 4, axis=0)
        dc = (d_prod * f_os[zr]).astype(BF16)
        do = (d_prod * f_cs[zr]).astype(BF16)
        part = dot_t(do, hot_rows[zr - 1])
        if zr == 1:
            dfeat[:, : 3 * wide] = part
            if cz > 3:
                dfeat[:, 3 * wide :] = jnp.zeros((4 * ch, (cz - 3) * wide), F32)
        else:
            dfeat[:, (zr - 1) * wide : (zr + 2) * wide] += part
        for t, i in enumerate(ids_of(zr)):
            dfeat[:, i * n : (i + 1) * n] += dot_t(dc[:, t * n : (t + 1) * n], ct[i])
    for zr in inner_rows:
        for t, i in enumerate(ids_of(zr)):
            raw = raws[zr][:, t * n : (t + 1) * n]
            env_grad[i : i + 1] = raw
            e_row = raw * geo[3, i : i + 1]
            e_hi = rounded(e_row)
            e_rows = jnp.where(row_8 == 0, e_hi, jnp.where(row_8 == 1, e_row - e_hi, 0.0)).astype(BF16)
            e_atom = dot_t(e_rows, ct[i])
            grad[0, zr - 1, t, 3:4] = -(e_atom[0:1] + e_atom[1:2])

    for zr in range(cz):
        ids = list(range(zr * cx, (zr + 1) * cx))
        span = slice(zr * wide, (zr + 1) * wide)
        dm = []
        for i in ids:
            hot_c = ct[i]
            fh, fl = split(dfeat[:, i * n : (i + 1) * n])
            dm.append(dot(jnp.concatenate([fh, fl], axis=1), jnp.concatenate([hot_c, hot_c], axis=0)))
        dm = join(dm, 1)
        w = wts[:, span]
        dw = dm[:ch]
        for m in range(3):
            piece = dm[(m + 1) * ch : (m + 2) * ch]
            dw = dw + piece * join([harm[m, i : i + 1] for i in ids], 1)
            d_h = jnp.sum(piece * w, axis=0, keepdims=True)
            for t, i in enumerate(ids):
                dharm[m, i : i + 1] = d_h[:, t * n : (t + 1) * n]
        dw = dw * join([rows_live[i : i + 1] for i in ids], 1)
        wh, wl = split(dw)
        parts = [wh, wl, wh]
        if kpad:
            parts.append(jnp.zeros((kpad, wide), BF16))
        d_lat = dot(env3, jnp.concatenate(parts, axis=0))
        if 1 <= zr <= bz:
            side = jnp.zeros((lat, n), F32)
            d_lat = d_lat + jnp.concatenate([side, dlat_own[zr - 1], side], axis=1)
        dh, dl = split(d_lat * dsilu[:, span])
        d_r = dot(wr3, jnp.concatenate([dh, dl, dh], axis=0))
        for t, i in enumerate(ids):
            drad[:, i, :] = d_r[:nb, t * n : (t + 1) * n]

    sum_s = drad[0] * sins[0]
    sum_c = drad[0] * coss[0]
    for k in range(1, nb):
        sum_s = sum_s + drad[k] * sins[k]
        sum_c = sum_c + (k + 1.0) * (drad[k] * coss[k])
    r = [geo[m] for m in range(3)]
    inv, env_slope = geo[4], geo[5]
    scale = inv * geo[3]
    d_dist = (
        (math.pi / CUTOFF) * sum_c * scale
        - sum_s * scale * inv
        + (sum_s * inv + env_grad[...]) * env_slope
    )
    for m in range(3):
        d_dist = d_dist - dharm[m] * r[m] * (inv * inv)
    gr[...] = jnp.zeros_like(gr)
    for m in range(3):
        d_m = d_dist * harm[m] + dharm[m] * inv
        hi = rounded(d_m)
        gr[:, m, :] = hi
        gr[:, m + 4, :] = d_m - hi

    second = {}

    def give(ready):
        for key, s in others_list:
            if s in second or not ready(s):
                continue
            i = index[s]
            second[s] = pltpu.make_async_remote_copy(
                src_ref=grad.at[s], dst_ref=back.at[i], send_sem=send2.at[i],
                recv_sem=recv2.at[i], device_id=owner(key), device_id_type=MESH,
            )
            second[s].start()

    order = sorted(range(total), key=lambda i: (-cells[i][0], cells[i][1]))
    targets = [
        {place(cells[i][0] + dz, cells[i][1] + dx)[0] for dz in (-1, 0, 1) for dx in (-1, 0, 1)}
        for i in order]
    for turn, i in enumerate(order):
        a, b = cells[i]
        g8 = gr[i]
        p = rows_p[i : i + 1]
        at_c = dot_t(jnp.concatenate([g8, jnp.zeros_like(g8)], axis=0).astype(BF16), ct[i])
        stack = [jnp.where(p == off, g8, 0.0) for off in range(9)] + [jnp.zeros_like(g8)]
        at_o = dot_t(jnp.concatenate(stack, axis=0).astype(BF16), ot[i])
        s, y, x = place(a, b)
        grad[s, y, x] -= at_c[:8]
        for off in range(9):
            s, y, x = place(a + off // 3 - 1, b + off % 3 - 1)
            grad[s, y, x] += at_o[8 * off : 8 * off + 8]
        if turn + 1 < total and b == cells[-1][1]:
            later = set().union(*targets[turn + 1 :])
            give(lambda s: s not in later)
    give(lambda s: True)
    for copy in second.values():
        copy.wait()
    for a in range(bz):
        for b in range(bx):
            acc = grad[mine, a, b]
            for s in range(len(others_list)):
                acc = acc + back[s, a, b]
            result_ref[:, a, b, :] = -(acc[:4] + acc[4:])


def solution(mesh):
    nz, nx = mesh.shape["gz"], mesh.shape["xy"]

    def body(coords, species, centers, others, live_count, in_weight, env_weight, up_weight, out_weight):
        _, bz, bx, n = coords.shape
        lat, ch = env_weight.shape
        nb = 8
        spec = (in_weight.shape[0] - nb) // 2
        cells = (bz + 2) * (bx + 2)
        ns = len(neighbours(nz, nx)) - 1
        vmem = lambda shape, dtype=F32: pltpu.VMEM(shape, dtype)
        args = (coords, species, centers, others, live_count, in_weight, env_weight.T, up_weight,
                out_weight[None])
        scratch = [vmem(x.shape, x.dtype) for x in args] + [
            vmem((ns + 1, bz, bx, 8, n)),
            vmem((3 * bz, 3 * bx, 16, n), BF16),
            vmem((cells, n, n), BF16),
            vmem((cells, n, n), BF16),
            vmem((bz, 3 * (bx + 2) * n, bx * n), BF16),
            vmem((cells, n)),
            vmem((cells, n), jnp.int32),
            vmem((6, cells, n)),
            vmem((2 * spec, cells * n)),
            vmem((nb, cells, n)),
            vmem((nb, cells, n)),
            vmem((nb, cells, n)),
            vmem((3, cells, n)),
            vmem((bz, 2, lat, bx * n), BF16),
            vmem((lat, cells * n)),
            vmem((ch, cells * n)),
            vmem((4 * ch, cells * n), BF16),
            vmem((4 * ch, cells * n)),
            vmem((bz, lat, bx * n)),
            vmem((cells, n)),
            vmem((3, cells, n)),
            vmem((nb, cells, n)),
            vmem((cells, 8, n)),
            vmem((ns + 1, bz, bx, 8, n)),
            vmem((ns, bz, bx, 8, n)),
        ] + [pltpu.SemaphoreType.DMA((ns,)) for _ in range(4)]
        scratch.append(pltpu.SemaphoreType.DMA((len(args),)))
        specs = [pl.BlockSpec(memory_space=pl.ANY) for _ in args]
        result = pl.pallas_call(
            functools.partial(kernel, nz, nx, bz, bx, nb, spec, ch, lat),
            out_shape=pltpu.VMEM((4, bz, bx, n), F32),
            in_specs=specs,
            out_specs=pl.BlockSpec(memory_space=pltpu.VMEM),
            scratch_shapes=scratch,
            compiler_params=pltpu.CompilerParams(collective_id=0, has_side_effects=True),
        )(*args)
        return result[3], result[:3]

    in_specs = (
        P(None, "gz", "xy", None), P("gz", "xy", None), P("gz", "xy", None), P("gz", "xy", None),
        P("gz", "xy"), P(), P(), P(), P(),
    )
    out_specs = (P("gz", "xy", None), P(None, "gz", "xy", None))
    return jax.shard_map(body, mesh=mesh, in_specs=in_specs, out_specs=out_specs, check_vma=False)
```

```python
import functools
import math

import jax
import jax.numpy as jnp
from jax import lax
from jax.experimental import pallas as pl
from jax.experimental.pallas import tpu as pltpu
from jax.sharding import PartitionSpec as P

SOFTEN = 0.01
CUTOFF = 3.5
F32 = jnp.float32
BF16 = jnp.bfloat16
MESH = pl.DeviceIdType.MESH


def rounded(x):
    return x.astype(BF16).astype(F32)


def split(x):
    high = x.astype(BF16)
    return high, (x - high.astype(F32)).astype(BF16)


def dot(a, b):
    return jnp.dot(a, b, preferred_element_type=F32)


def dot_t(a, b):
    return lax.dot_general(a, b, (((1,), (1,)), ((), ())), preferred_element_type=F32)


def join(parts, axis):
    return parts[0] if len(parts) == 1 else jnp.concatenate(parts, axis=axis)


def neighbours(nz, nx):
    slots = {(0, 0): 0}
    for dz in (-1, 0, 1):
        for dx in (-1, 0, 1):
            slots.setdefault((dz % nz, dx % nx), len(slots))
    return slots


def kernel(
    nz, nx, bz, bx, nb, spec, ch, lat,
    coords_hbm, species_hbm, centers_hbm, others_hbm, live_hbm, in_hbm, env_hbm, up_hbm, out_hbm,
    result_ref,
    coords_ref, species_ref, centers_ref, others_ref, live_ref, in_ref, env_ref, up_ref, out_ref,
    atoms, edges, tab, hot, hot_t, rows_hot, rows_hot_t, codes, rows_c, rows_o, rows_p, rows_live,
    diffs, geo, xs, sins, coss, rad, harm,
    l2, dsilu, wts, feat, dfeat, dlat_own, env_grad, dharm, drad, gr, grad, give_ref, back,
    send1, recv1, send2, recv2, send3, recv3, load_sem,
):
    n = coords_ref.shape[-1]
    slots = neighbours(nz, nx)
    me_z, me_x = lax.axis_index("gz"), lax.axis_index("xy")
    mine = slots[(1 % nz, 0)]
    others_list = [(key, s) for key, s in slots.items() if s != mine]
    index = {s: i for i, (_, s) in enumerate(others_list)}

    def owner(key):
        return (lax.rem(me_z + (key[0] - 1) % nz, nz), lax.rem(me_x + key[1], nx))

    def user(key):
        return (lax.rem(me_z + (1 - key[0]) % nz, nz), lax.rem(me_x + (-key[1]) % nx, nx))

    barrier = pltpu.get_barrier_semaphore()
    for key, _ in others_list:
        pl.semaphore_signal(barrier, inc=1, device_id=owner(key), device_id_type=MESH)

    loads = [
        pltpu.make_async_copy(source, target, load_sem.at[k])
        for k, (source, target) in enumerate([
            (coords_hbm, coords_ref), (species_hbm, species_ref), (centers_hbm, centers_ref),
            (others_hbm, others_ref), (live_hbm, live_ref), (in_hbm, in_ref), (env_hbm, env_ref),
            (up_hbm, up_ref), (out_hbm, out_ref)])
    ]
    for load in loads:
        load.start()
    for load in loads[:5]:
        load.wait()
    lane = lax.broadcasted_iota(jnp.int32, (1, n), 1)
    for a in range(bz):
        for b in range(bx):
            code = centers_ref[a, b : b + 1, :] + 128 * others_ref[a, b : b + 1, :]
            code = jnp.where(lane < live_ref[a : a + 1, b : b + 1], code, -1)
            edges[mine, a, b : b + 1, :] = code.astype(F32)
            atoms[mine, a, b] = jnp.concatenate(
                [coords_ref[:, a, b, :], species_ref[a, b : b + 1, :].astype(F32)], axis=0)
    pl.semaphore_wait(barrier, len(others_list))
    first = {}
    for key, s in others_list:
        i = index[s]
        for ref, send, recv in ((atoms, send1, recv1), (edges, send3, recv3)):
            copy = pltpu.make_async_remote_copy(
                src_ref=ref.at[mine], dst_ref=ref.at[s], send_sem=send.at[i],
                recv_sem=recv.at[i], device_id=user(key), device_id_type=MESH,
            )
            copy.start()
            first.setdefault(key, []).append(copy)

    for load in loads[5:]:
        load.wait()
    w_in = in_ref[...]
    w_hi = rounded(w_in)
    w_lo = w_in - w_hi
    gap = jnp.zeros((nb, lat), F32)
    kin = 4 * nb + 4 * spec
    w_rows = [w_hi[:nb], w_hi[:nb], w_lo[:nb], gap, w_hi[nb:], w_lo[nb:]]
    if lat > kin:
        w_rows.append(jnp.zeros((lat - kin, lat), F32))
    in_t = jnp.concatenate(w_rows, axis=0).T.astype(BF16)[:, :kin]
    wr2 = jnp.concatenate(
        [jnp.concatenate([w_hi[:nb], w_hi[:nb]], axis=1), jnp.concatenate([w_lo[:nb], gap], axis=1)],
        axis=0).astype(BF16)
    env_t = env_ref[...]
    et_hi = rounded(env_t)
    et_lo = env_t - et_hi
    env_t2 = jnp.concatenate(
        [jnp.concatenate([et_hi, et_hi], axis=1), jnp.concatenate([et_lo, jnp.zeros_like(et_lo)], axis=1)],
        axis=0).astype(BF16)
    kpad = -(3 * ch) % lat
    env3 = jnp.concatenate(
        [et_hi, et_hi, et_lo] + ([jnp.zeros((kpad, lat), F32)] if kpad else []), axis=0
    ).T.astype(BF16)
    up = up_ref[...]
    up_hi = rounded(up)
    up_lo = up - up_hi
    up3 = jnp.concatenate([up_hi, up_hi, up_lo], axis=1).astype(BF16)
    up_t = jnp.concatenate(
        [x.T.astype(BF16) for x in (up_hi[:lat], up_hi[:lat], up_lo[:lat])]
        + [jnp.concatenate(
            [up_hi[lat:], up_hi[lat:], up_lo[lat:]]
            + ([jnp.zeros((kpad, lat), F32)] if kpad else []), axis=0).T.astype(BF16)],
        axis=1)
    out_col = jnp.broadcast_to(out_ref[...], (n, lat)).T

    rows_hot[...] = jnp.zeros_like(rows_hot)
    rows_hot_t[...] = jnp.zeros_like(rows_hot_t)
    grad[...] = jnp.zeros_like(grad)
    cz, cx = bz + 2, bx + 2
    total = cz * cx
    wide = cx * n
    inner = bx * n
    cells = [(a, b) for a in range(bz - 1, 2 * bz + 1) for b in range(bx - 1, 2 * bx + 1)]
    row_n = lax.broadcasted_iota(jnp.int32, (n, n), 0).astype(F32).astype(BF16)
    row_s = lax.broadcasted_iota(jnp.int32, (spec, n), 0).astype(F32)
    one, zero = jnp.ones((n, n), BF16), jnp.zeros((n, n), BF16)

    def place(a, b):
        return slots[((a // bz - 1) % nz, (b // bx - 1) % nx)], a % bz, b % bx

    def tables(rows):
        for a in rows:
            hl = {}
            for b in range(bx - 2, 2 * bx + 2):
                s, i, j = place(a, b)
                part = atoms[s, i, j]
                hi = rounded(part)
                hl[b] = jnp.concatenate([hi, part - hi], axis=0)
            for b in range(bx - 1, 2 * bx + 1):
                tab[a, b] = jnp.concatenate(
                    [hl[b - 1], hl[b], hl[b + 1], jnp.zeros((8, n), F32)], axis=0).astype(BF16)

    def decode(rows):
        c = slice(rows[0] * cx, (rows[-1] + 1) * cx)
        for i in range(rows[0] * cx, (rows[-1] + 1) * cx):
            s, y, x = place(*cells[i])
            codes[i : i + 1] = edges[s, y, x : x + 1, :]
        code = codes[c].astype(jnp.int32)
        o = code >> 7
        rows_c[c] = (code & 127).astype(F32)
        rows_o[c] = (o & 127).astype(F32)
        rows_p[c] = o >> 7
        rows_live[c] = (code >= 0).astype(F32)

    def gather(i):
        a, b = cells[i]
        p = rows_p[i : i + 1]
        hot_c = jnp.where(row_n == rows_c[i : i + 1].astype(BF16), one, zero)
        hot_o = jnp.where(row_n == rows_o[i : i + 1].astype(BF16), one, zero)
        both = jnp.concatenate([hot_c, hot_o], axis=1)
        hot[i] = both
        hot_t[i] = jnp.concatenate([hot_c.T, hot_o.T], axis=1)
        zr, xc = i // cx, i % cx
        if 1 <= zr <= bz and 1 <= xc <= bx:
            for dz in range(3):
                for dx in range(3):
                    col = dz * cx + xc - 1 + dx
                    masked = hot_o * (p == 3 * dz + dx).astype(F32).astype(BF16)
                    rows_hot[zr - 1, col * n : (col + 1) * n, (xc - 1) * n : xc * n] = masked
                    rows_hot_t[zr - 1, (xc - 1) * n : xc * n, col * n : (col + 1) * n] = masked.T
        around = jnp.concatenate([tab[a + dz, b] for dz in (-1, 0, 1)], axis=0)
        got = dot(around, both)
        at_c = got[40:48, :n]
        at_o = jnp.zeros((8, n), F32)
        for dz in range(3):
            for dx in range(3):
                at_o = jnp.where(p == 3 * dz + dx, got[32 * dz + 8 * dx : 32 * dz + 8 * dx + 8, n:], at_o)
        at_c = at_c[:4] + at_c[4:]
        at_o = at_o[:4] + at_o[4:]
        diffs[i] = at_o - at_c
        xs[:, i * n : (i + 1) * n] = jnp.concatenate(
            [(row_s == at_c[3:4]).astype(F32), (row_s == at_o[3:4]).astype(F32)], axis=0).astype(BF16)

    def geometry(rows):
        c = slice(rows[0] * cx, (rows[-1] + 1) * cx)
        p = rows_p[c]
        third = (p >= 3).astype(jnp.int32) + (p >= 6).astype(jnp.int32)
        r = [
            diffs[c, 0, :] + (third - 1).astype(F32),
            diffs[c, 1, :] + (p - 3 * third - 1).astype(F32),
            diffs[c, 2, :],
        ]
        dist = jnp.sqrt(r[0] * r[0] + r[1] * r[1] + r[2] * r[2] + SOFTEN)
        inv = 1.0 / dist
        q = dist / CUTOFF
        rest = 1.0 - q * q
        envelope = rest * rest
        scale = inv * envelope
        s1 = jnp.sin(math.pi * q)
        c1 = jnp.cos(math.pi * q)
        s0, c0, sk, ck = jnp.zeros_like(s1), jnp.ones_like(c1), s1, c1
        for k in range(nb):
            sins[k, c] = sk
            coss[k, c] = ck
            rad[k, c] = sk * scale
            s0, sk = sk, 2.0 * c1 * sk - s0
            c0, ck = ck, 2.0 * c1 * ck - c0
        for m in range(3):
            harm[m, c] = r[m] * inv
            geo[m, c] = r[m]
        env_grad[c] = jnp.zeros_like(q)
        geo[3, c] = envelope
        geo[4, c] = inv
        geo[5, c] = (-4.0 / CUTOFF) * q * rest

    def ids_of(zr):
        return list(range(zr * cx, (zr + 1) * cx))

    def inner_of(zr):
        return ids_of(zr)[1:-1]

    def latents(rows):
        pres, lows, mls = {}, {}, {}
        for zr in rows:
            span = slice(zr * wide, (zr + 1) * wide)
            radial = join([rad[:, i, :] for i in ids_of(zr)], 1)
            rh = rounded(radial)
            x_s = xs[:, span]
            pres[zr] = dot(in_t, jnp.concatenate([
                jnp.concatenate([rh, radial - rh], axis=0).astype(BF16),
                jnp.concatenate([rh, jnp.zeros_like(rh)], axis=0).astype(BF16), x_s, x_s], axis=0))
        for zr in rows:
            span = slice(zr * wide, (zr + 1) * wide)
            pre = pres[zr]
            sig = 0.5 + 0.5 * jnp.tanh(0.5 * pre)
            latent = pre * sig
            dsilu[:, span] = sig + latent * (1.0 - sig)
            lh, ll = split(latent)
            if 1 <= zr <= bz:
                l2[zr - 1, 0] = lh[:, n : n + inner]
                l2[zr - 1, 1] = ll[:, n : n + inner]
            lows[zr] = dot(env_t2, jnp.concatenate([lh, ll], axis=0))
        for zr in rows:
            span = slice(zr * wide, (zr + 1) * wide)
            ids = ids_of(zr)
            w = lows[zr]
            w = (w[:ch] + w[ch:]) * join([rows_live[i : i + 1] for i in ids], 1)
            wts[:, span] = w
            msgs = jnp.concatenate(
                [w] + [w * join([harm[m, i : i + 1] for i in ids], 1) for m in range(3)], axis=0)
            mls[zr] = split(msgs)
            mh, ml = mls[zr]
            for t, i in enumerate(ids):
                cut = slice(t * n, (t + 1) * n)
                hot_c = hot_t[i, :, :n]
                feat[:, i * n : (i + 1) * n] = dot(
                    jnp.concatenate([mh[:, cut], ml[:, cut]], axis=1),
                    jnp.concatenate([hot_c, hot_c], axis=0)).astype(BF16)

    early, late = list(range(2, cz)), [0, 1]
    for copies in first.values():
        for copy in copies:
            copy.wait()
    every = list(range(cz))
    decode(every)
    tables(range(bz - 2, 2 * bz + 2))
    for i in range(total):
        gather(i)
    geometry(every)
    latents(every)

    row_16 = lax.broadcasted_iota(jnp.int32, (16, n), 0)
    out_rows = jnp.concatenate([out_col] * bx, axis=1)
    inner_rows = range(1, bz + 1)
    f_cs, f_os, us, joins, raws = {}, {}, {}, {}, {}
    for zr in inner_rows:
        f_cs[zr] = join([dot(feat[:, i * n : (i + 1) * n], hot[i, :, :n]) for i in inner_of(zr)], 1)
        f_os[zr] = dot(feat[:, (zr - 1) * wide : (zr + 2) * wide], rows_hot[zr - 1])
    for zr in inner_rows:
        prod4 = f_cs[zr] * f_os[zr]
        prod = prod4[:ch] + prod4[ch : 2 * ch] + prod4[2 * ch : 3 * ch] + prod4[3 * ch :]
        ph, pl_ = split(prod)
        parts = [l2[zr - 1, 0], l2[zr - 1, 1], l2[zr - 1, 0], ph, pl_, ph]
        if kpad:
            parts.append(jnp.zeros((kpad, inner), BF16))
        us[zr] = dot(up_t, jnp.concatenate(parts, axis=0))
    for zr in inner_rows:
        env_row = join([geo[3, i : i + 1] for i in inner_of(zr)], 1)
        alive = join([rows_live[i : i + 1] for i in inner_of(zr)], 1)
        u = us[zr]
        sig = 0.5 + 0.5 * jnp.tanh(0.5 * u)
        hid = u * sig
        raws[zr] = jnp.sum(out_rows * hid, axis=0, keepdims=True) * alive
        d_u = out_rows * (alive * env_row) * (sig + hid * (1.0 - sig))
        dh, dl = split(d_u)
        joins[zr] = dot(up3, jnp.concatenate([dh, dl, dh], axis=0))
    for zr in inner_rows:
        d_join = joins[zr]
        dlat_own[zr - 1] = d_join[:lat]
        d_prod = jnp.concatenate([d_join[lat:]] * 4, axis=0)
        dch, dcl = split(d_prod * f_os[zr])
        doh, dol = split(d_prod * f_cs[zr])
        turned_rows = rows_hot_t[zr - 1]
        part = dot(jnp.concatenate([doh, dol], axis=1), jnp.concatenate([turned_rows, turned_rows], axis=0))
        if zr == 1:
            dfeat[:, : 3 * wide] = part
            if cz > 3:
                dfeat[:, 3 * wide :] = jnp.zeros((4 * ch, (cz - 3) * wide), F32)
        else:
            dfeat[:, (zr - 1) * wide : (zr + 2) * wide] += part
        for t, i in enumerate(inner_of(zr)):
            raw = raws[zr][:, t * n : (t + 1) * n]
            env_grad[i : i + 1] = raw
            e_row = raw * geo[3, i : i + 1]
            e_hi = rounded(e_row)
            e_lo = jnp.where(row_16 == 0, e_row - e_hi, 0.0).astype(BF16)
            e_hi = jnp.where(row_16 == 0, e_hi, 0.0).astype(BF16)
            cut = slice(t * n, (t + 1) * n)
            hot_c = hot_t[i, :, :n]
            both = dot(
                jnp.concatenate([
                    jnp.concatenate([dch[:, cut], e_hi], axis=0),
                    jnp.concatenate([dcl[:, cut], e_lo], axis=0)], axis=1),
                jnp.concatenate([hot_c, hot_c], axis=0))
            dfeat[:, i * n : (i + 1) * n] += both[: 4 * ch]
            grad[0, zr - 1, t, 3:4] = -both[4 * ch : 4 * ch + 1]

    def backward(rows):
        dms, dls = {}, {}
        for zr in rows:
            dm = []
            for i in ids_of(zr):
                hot_c = hot[i, :, :n]
                fh, fl = split(dfeat[:, i * n : (i + 1) * n])
                dm.append(dot(jnp.concatenate([fh, fl], axis=1), jnp.concatenate([hot_c, hot_c], axis=0)))
            dms[zr] = join(dm, 1)
        for zr in rows:
            ids = ids_of(zr)
            dm = dms[zr]
            dw = dm[:ch]
            for m in range(3):
                dw = dw + dm[(m + 1) * ch : (m + 2) * ch] * join([harm[m, i : i + 1] for i in ids], 1)
            dw = dw * join([rows_live[i : i + 1] for i in ids], 1)
            wh, wl = split(dw)
            parts = [wh, wl, wh]
            if kpad:
                parts.append(jnp.zeros((kpad, wide), BF16))
            dls[zr] = dot(env3, jnp.concatenate(parts, axis=0))
        for zr in rows:
            span = slice(zr * wide, (zr + 1) * wide)
            d_lat = dls[zr]
            if 1 <= zr <= bz:
                side = jnp.zeros((lat, n), F32)
                d_lat = d_lat + jnp.concatenate([side, dlat_own[zr - 1], side], axis=1)
            dh, dl = split(d_lat * dsilu[:, span])
            d_r = dot(wr2, jnp.concatenate([dh, dl], axis=0))
            d_r = d_r[:nb] + d_r[nb:]
            for t, i in enumerate(ids_of(zr)):
                drad[:, i, :] = d_r[:, t * n : (t + 1) * n]
        for zr in rows:
            span = slice(zr * wide, (zr + 1) * wide)
            w = wts[:, span]
            for m in range(3):
                d_h = jnp.sum(dms[zr][(m + 1) * ch : (m + 2) * ch] * w, axis=0, keepdims=True)
                for t, i in enumerate(ids_of(zr)):
                    dharm[m, i : i + 1] = d_h[:, t * n : (t + 1) * n]

    def radial_backward(rows):
        c = slice(rows[0] * cx, (rows[-1] + 1) * cx)
        sum_s = drad[0, c] * sins[0, c]
        sum_c = drad[0, c] * coss[0, c]
        for k in range(1, nb):
            sum_s = sum_s + drad[k, c] * sins[k, c]
            sum_c = sum_c + (k + 1.0) * (drad[k, c] * coss[k, c])
        inv, env_slope = geo[4, c], geo[5, c]
        scale = inv * geo[3, c]
        d_dist = (
            (math.pi / CUTOFF) * sum_c * scale
            - sum_s * scale * inv
            + (sum_s * inv + env_grad[c]) * env_slope
        )
        for m in range(3):
            d_dist = d_dist - dharm[m, c] * geo[m, c] * (inv * inv)
        for m in range(3):
            d_m = d_dist * harm[m, c] + dharm[m, c] * inv
            hi = rounded(d_m)
            gr[c, m, :] = hi
            gr[c, m + 4, :] = d_m - hi
        gr[c, 3, :] = jnp.zeros_like(inv)
        gr[c, 7, :] = jnp.zeros_like(inv)

    def scatter(i):
        a, b = cells[i]
        g8 = gr[i]
        p = rows_p[i : i + 1]
        stack = [g8] + [jnp.where(p == off, g8, 0.0) for off in range(9)]
        out = dot(jnp.concatenate(stack, axis=0).astype(BF16), hot_t[i])
        s, y, x = place(a, b)
        grad[s, y, x] -= out[:8, :n]
        for off in range(9):
            s, y, x = place(a + off // 3 - 1, b + off % 3 - 1)
            grad[s, y, x] += out[8 + 8 * off : 16 + 8 * off, n:]

    second = {}

    def give(later):
        for key, s in others_list:
            if s in second or s in later:
                continue
            i = index[s]
            for y in range(bz):
                for x in range(bx):
                    acc = grad[s, y, x]
                    give_ref[i, y, x] = acc[:4] + acc[4:]
            second[s] = pltpu.make_async_remote_copy(
                src_ref=give_ref.at[i], dst_ref=back.at[i], send_sem=send2.at[i],
                recv_sem=recv2.at[i], device_id=owner(key), device_id_type=MESH,
            )
            second[s].start()

    def targets(rows):
        return {
            place(cells[i][0] + dz, cells[i][1] + dx)[0]
            for zr in rows for i in ids_of(zr) for dz in (-1, 0, 1) for dx in (-1, 0, 1)}

    backward(early[::-1])
    radial_backward(early)
    for zr in reversed(early):
        for i in ids_of(zr):
            scatter(i)
    give(targets(late))
    backward(late[::-1])
    radial_backward(late)
    for zr in reversed(late):
        for i in ids_of(zr):
            scatter(i)
    give(set())
    for copy in second.values():
        copy.wait()
    for a in range(bz):
        for b in range(bx):
            acc = grad[mine, a, b]
            acc = acc[:4] + acc[4:]
            for s in range(len(others_list)):
                acc = acc + back[s, a, b]
            result_ref[:, a, b, :] = -acc


def deliver(result_ref, energy_ref, force_ref, sem):
    copies = [
        pltpu.make_async_copy(result_ref.at[3], energy_ref, sem.at[0]),
        pltpu.make_async_copy(result_ref.at[pl.ds(0, 3)], force_ref, sem.at[1]),
    ]
    for copy in copies:
        copy.start()
    for copy in copies:
        copy.wait()


def solution(mesh):
    nz, nx = mesh.shape["gz"], mesh.shape["xy"]

    def body(coords, species, centers, others, live_count, in_weight, env_weight, up_weight, out_weight):
        _, bz, bx, n = coords.shape
        lat, ch = env_weight.shape
        nb = 8
        spec = (in_weight.shape[0] - nb) // 2
        cells = (bz + 2) * (bx + 2)
        ns = len(neighbours(nz, nx)) - 1
        vmem = lambda shape, dtype=F32: pltpu.VMEM(shape, dtype)
        args = (coords, species, centers, others, live_count, in_weight, env_weight.T, up_weight,
                out_weight[None])
        scratch = [vmem(x.shape, x.dtype) for x in args] + [
            vmem((ns + 1, bz, bx, 4, n)),
            vmem((ns + 1, bz, bx, n)),
            vmem((3 * bz, 3 * bx, 32, n), BF16),
            vmem((cells, n, 2 * n), BF16),
            vmem((cells, n, 2 * n), BF16),
            vmem((bz, 3 * (bx + 2) * n, bx * n), BF16),
            vmem((bz, bx * n, 3 * (bx + 2) * n), BF16),
            vmem((cells, n)),
            vmem((cells, n)),
            vmem((cells, n)),
            vmem((cells, n), jnp.int32),
            vmem((cells, n)),
            vmem((cells, 4, n)),
            vmem((6, cells, n)),
            vmem((2 * spec, cells * n), BF16),
            vmem((nb, cells, n)),
            vmem((nb, cells, n)),
            vmem((nb, cells, n)),
            vmem((3, cells, n)),
            vmem((bz, 2, lat, bx * n), BF16),
            vmem((lat, cells * n)),
            vmem((ch, cells * n)),
            vmem((4 * ch, cells * n), BF16),
            vmem((4 * ch, cells * n)),
            vmem((bz, lat, bx * n)),
            vmem((cells, n)),
            vmem((3, cells, n)),
            vmem((nb, cells, n)),
            vmem((cells, 8, n)),
            vmem((ns + 1, bz, bx, 8, n)),
            vmem((ns, bz, bx, 4, n)),
            vmem((ns, bz, bx, 4, n)),
        ] + [pltpu.SemaphoreType.DMA((ns,)) for _ in range(6)]
        scratch.append(pltpu.SemaphoreType.DMA((len(args),)))
        specs = [pl.BlockSpec(memory_space=pl.ANY) for _ in args]
        result = pl.pallas_call(
            functools.partial(kernel, nz, nx, bz, bx, nb, spec, ch, lat),
            out_shape=pltpu.VMEM((4, bz, bx, n), F32),
            in_specs=specs,
            out_specs=pl.BlockSpec(memory_space=pltpu.VMEM),
            scratch_shapes=scratch,
            compiler_params=pltpu.CompilerParams(collective_id=0, has_side_effects=True),
        )(*args)
        return pl.pallas_call(
            deliver,
            out_shape=(jax.ShapeDtypeStruct((bz, bx, n), F32), jax.ShapeDtypeStruct((3, bz, bx, n), F32)),
            in_specs=[pl.BlockSpec(memory_space=pltpu.VMEM)],
            out_specs=(pl.BlockSpec(memory_space=pl.ANY), pl.BlockSpec(memory_space=pl.ANY)),
            scratch_shapes=[pltpu.SemaphoreType.DMA((2,))],
        )(pltpu.with_memory_space_constraint(result, pltpu.VMEM))

    in_specs = (
        P(None, "gz", "xy", None), P("gz", "xy", None), P("gz", "xy", None), P("gz", "xy", None),
        P("gz", "xy"), P(), P(), P(), P(),
    )
    out_specs = (P("gz", "xy", None), P(None, "gz", "xy", None))
    return jax.shard_map(body, mesh=mesh, in_specs=in_specs, out_specs=out_specs, check_vma=False)
```

```python
import functools
import math

import jax
import jax.numpy as jnp
from jax import lax
from jax.experimental import pallas as pl
from jax.experimental.pallas import tpu as pltpu
from jax.sharding import PartitionSpec as P

SOFTEN = 0.01
CUTOFF = 3.5
F32 = jnp.float32
BF16 = jnp.bfloat16
MESH = pl.DeviceIdType.MESH


def rounded(x):
    return x.astype(BF16).astype(F32)


def split(x):
    high = x.astype(BF16)
    return high, (x - high.astype(F32)).astype(BF16)


def dot(a, b):
    return jnp.dot(a, b, preferred_element_type=F32)


def dot_t(a, b):
    return lax.dot_general(a, b, (((1,), (1,)), ((), ())), preferred_element_type=F32)


def join(parts, axis):
    return parts[0] if len(parts) == 1 else jnp.concatenate(parts, axis=axis)


def neighbours(nz, nx):
    slots = {(0, 0): 0}
    for dz in (-1, 0, 1):
        for dx in (-1, 0, 1):
            slots.setdefault((dz % nz, dx % nx), len(slots))
    return slots


def kernel(
    nz, nx, bz, bx, nb, spec, ch, lat,
    coords_hbm, species_hbm, centers_hbm, others_hbm, live_hbm, in_hbm, env_hbm, up_hbm, out_hbm,
    result_ref,
    coords_ref, ints_ref, live_ref, weights_ref, out_ref,
    atoms, edges, tab, hot, hot_t, rows_hot, rows_hot_t, codes, rows_c, rows_o, rows_p, rows_live,
    diffs, geo, xs, sins, coss, rad, harm,
    l2, dsilu, wts, feat, dfeat, dlat_own, env_grad, dharm, drad, gr, grad, give_ref, back,
    send_sem, recv_sem, load_sem,
):
    n = coords_ref.shape[-1]
    slots = neighbours(nz, nx)
    me_z, me_x = lax.axis_index("gz"), lax.axis_index("xy")
    mine = slots[(1 % nz, 0)]
    last = len(slots) - 1
    slots = {key: last if s == mine else mine if s == last else s for key, s in slots.items()}
    mine = last
    centre = slots[(0, 0)]
    others_list = [(key, s) for key, s in slots.items() if s != mine]
    index = {s: i for i, (_, s) in enumerate(others_list)}

    def owner(key):
        return (lax.rem(me_z + (key[0] - 1) % nz, nz), lax.rem(me_x + key[1], nx))

    def user(key):
        return (lax.rem(me_z + (1 - key[0]) % nz, nz), lax.rem(me_x + (-key[1]) % nx, nx))

    barrier = pltpu.get_barrier_semaphore()
    for key, _ in others_list:
        pl.semaphore_signal(barrier, inc=1, device_id=owner(key), device_id_type=MESH)

    def whole(ref, sem):
        pltpu.make_async_copy(ref, ref, sem).wait()

    for k, (source, target) in enumerate([
            (coords_hbm, coords_ref), (live_hbm, live_ref), (out_hbm, out_ref)]):
        pltpu.make_async_copy(source, target, load_sem.at[k]).start()
    for k, source in enumerate((species_hbm, centers_hbm, others_hbm)):
        pltpu.make_async_copy(source, ints_ref.at[k], load_sem.at[3]).start()
    rows_in, rows_env, rows_up = in_hbm.shape[0], env_hbm.shape[0], up_hbm.shape[0]
    row = 0
    for source in (in_hbm, env_hbm, up_hbm):
        pltpu.make_async_copy(source, weights_ref.at[pl.ds(row, source.shape[0])], load_sem.at[4]).start()
        row += source.shape[0]
    whole(coords_ref, load_sem.at[0])
    whole(live_ref, load_sem.at[1])
    whole(ints_ref, load_sem.at[3])
    lane = lax.broadcasted_iota(jnp.int32, (1, n), 1)
    for a in range(bz):
        for b in range(bx):
            code = ints_ref[1, a, b : b + 1, :] + 128 * ints_ref[2, a, b : b + 1, :]
            code = jnp.where(lane < live_ref[a : a + 1, b : b + 1], code, -1)
            edges[mine, a, b : b + 1, :] = code.astype(F32)
            atoms[mine, a, b] = jnp.concatenate(
                [coords_ref[:, a, b, :], ints_ref[0, a, b : b + 1, :].astype(F32)], axis=0)
    pl.semaphore_wait(barrier, len(others_list))
    for key, s in others_list:
        for k, ref in enumerate((atoms, edges)):
            pltpu.make_async_remote_copy(
                src_ref=ref.at[mine], dst_ref=ref.at[s], send_sem=send_sem.at[k],
                recv_sem=recv_sem.at[k], device_id=user(key), device_id_type=MESH,
            ).start()

    whole(out_ref, load_sem.at[2])
    whole(weights_ref, load_sem.at[4])
    w_in = weights_ref[:rows_in]
    w_hi = rounded(w_in)
    w_lo = w_in - w_hi
    gap = jnp.zeros((nb, lat), F32)
    kin = 4 * nb + 4 * spec
    w_rows = [w_hi[:nb], w_hi[:nb], w_lo[:nb], gap, w_hi[nb:], w_lo[nb:]]
    if lat > kin:
        w_rows.append(jnp.zeros((lat - kin, lat), F32))
    in_t = jnp.concatenate(w_rows, axis=0).T.astype(BF16)[:, :kin]
    wr2 = jnp.concatenate(
        [jnp.concatenate([w_hi[:nb], w_hi[:nb]], axis=1), jnp.concatenate([w_lo[:nb], gap], axis=1)],
        axis=0).astype(BF16)
    env_t = weights_ref[rows_in : rows_in + rows_env]
    et_hi = rounded(env_t)
    et_lo = env_t - et_hi
    env_t2 = jnp.concatenate(
        [jnp.concatenate([et_hi, et_hi], axis=1), jnp.concatenate([et_lo, jnp.zeros_like(et_lo)], axis=1)],
        axis=0).astype(BF16)
    kpad = -(3 * ch) % lat
    env3 = jnp.concatenate(
        [et_hi, et_hi, et_lo] + ([jnp.zeros((kpad, lat), F32)] if kpad else []), axis=0
    ).T.astype(BF16)
    up = weights_ref[rows_in + rows_env :]
    up_hi = rounded(up)
    up_lo = up - up_hi
    up3 = jnp.concatenate([up_hi, up_hi, up_lo], axis=1).astype(BF16)
    up_t = jnp.concatenate(
        [x.T.astype(BF16) for x in (up_hi[:lat], up_hi[:lat], up_lo[:lat])]
        + [jnp.concatenate(
            [up_hi[lat:], up_hi[lat:], up_lo[lat:]]
            + ([jnp.zeros((kpad, lat), F32)] if kpad else []), axis=0).T.astype(BF16)],
        axis=1)
    out_col = jnp.broadcast_to(out_ref[...], (n, lat)).T

    rows_hot[...] = jnp.zeros_like(rows_hot)
    rows_hot_t[...] = jnp.zeros_like(rows_hot_t)
    grad[...] = jnp.zeros_like(grad)
    cz, cx = bz + 2, bx + 2
    total = cz * cx
    wide = cx * n
    inner = bx * n
    cells = [(a, b) for a in range(bz - 1, 2 * bz + 1) for b in range(bx - 1, 2 * bx + 1)]
    row_n = lax.broadcasted_iota(jnp.int32, (n, n), 0).astype(F32).astype(BF16)
    row_s = lax.broadcasted_iota(jnp.int32, (spec, n), 0).astype(F32)
    one, zero = jnp.ones((n, n), BF16), jnp.zeros((n, n), BF16)

    def place(a, b):
        return slots[((a // bz - 1) % nz, (b // bx - 1) % nx)], a % bz, b % bx

    def tables(rows):
        for a in rows:
            hl = {}
            for b in range(bx - 2, 2 * bx + 2):
                s, i, j = place(a, b)
                part = atoms[s, i, j]
                hi = rounded(part)
                hl[b] = jnp.concatenate([hi, part - hi], axis=0)
            for b in range(bx - 1, 2 * bx + 1):
                tab[a, b] = jnp.concatenate(
                    [hl[b - 1], hl[b], hl[b + 1], jnp.zeros((8, n), F32)], axis=0).astype(BF16)

    def decode(rows):
        c = slice(rows[0] * cx, (rows[-1] + 1) * cx)
        for i in range(rows[0] * cx, (rows[-1] + 1) * cx):
            s, y, x = place(*cells[i])
            codes[i : i + 1] = edges[s, y, x : x + 1, :]
        code = codes[c].astype(jnp.int32)
        o = code >> 7
        rows_c[c] = (code & 127).astype(F32)
        rows_o[c] = (o & 127).astype(F32)
        rows_p[c] = o >> 7
        rows_live[c] = (code >= 0).astype(F32)

    def gather(i):
        a, b = cells[i]
        p = rows_p[i : i + 1]
        hot_c = jnp.where(row_n == rows_c[i : i + 1].astype(BF16), one, zero)
        hot_o = jnp.where(row_n == rows_o[i : i + 1].astype(BF16), one, zero)
        both = jnp.concatenate([hot_c, hot_o], axis=1)
        hot[i] = both
        hot_t[i] = jnp.concatenate([hot_c.T, hot_o.T], axis=1)
        zr, xc = i // cx, i % cx
        if 1 <= zr <= bz and 1 <= xc <= bx:
            for dz in range(3):
                for dx in range(3):
                    col = dz * cx + xc - 1 + dx
                    masked = hot_o * (p == 3 * dz + dx).astype(F32).astype(BF16)
                    rows_hot[zr - 1, col * n : (col + 1) * n, (xc - 1) * n : xc * n] = masked
                    rows_hot_t[zr - 1, (xc - 1) * n : xc * n, col * n : (col + 1) * n] = masked.T
        around = jnp.concatenate([tab[a + dz, b] for dz in (-1, 0, 1)], axis=0)
        got = dot(around, both)
        at_c = got[40:48, :n]
        at_o = jnp.zeros((8, n), F32)
        for dz in range(3):
            for dx in range(3):
                at_o = jnp.where(p == 3 * dz + dx, got[32 * dz + 8 * dx : 32 * dz + 8 * dx + 8, n:], at_o)
        at_c = at_c[:4] + at_c[4:]
        at_o = at_o[:4] + at_o[4:]
        diffs[i] = at_o - at_c
        xs[:, i * n : (i + 1) * n] = jnp.concatenate(
            [(row_s == at_c[3:4]).astype(F32), (row_s == at_o[3:4]).astype(F32)], axis=0).astype(BF16)

    def geometry(rows):
        c = slice(rows[0] * cx, (rows[-1] + 1) * cx)
        p = rows_p[c]
        third = (p >= 3).astype(jnp.int32) + (p >= 6).astype(jnp.int32)
        r = [
            diffs[c, 0, :] + (third - 1).astype(F32),
            diffs[c, 1, :] + (p - 3 * third - 1).astype(F32),
            diffs[c, 2, :],
        ]
        dist = jnp.sqrt(r[0] * r[0] + r[1] * r[1] + r[2] * r[2] + SOFTEN)
        inv = 1.0 / dist
        q = dist / CUTOFF
        rest = 1.0 - q * q
        envelope = rest * rest
        scale = inv * envelope
        s1 = jnp.sin(math.pi * q)
        c1 = jnp.cos(math.pi * q)
        s0, c0, sk, ck = jnp.zeros_like(s1), jnp.ones_like(c1), s1, c1
        for k in range(nb):
            sins[k, c] = sk
            coss[k, c] = ck
            rad[k, c] = sk * scale
            s0, sk = sk, 2.0 * c1 * sk - s0
            c0, ck = ck, 2.0 * c1 * ck - c0
        for m in range(3):
            harm[m, c] = r[m] * inv
            geo[m, c] = r[m]
        env_grad[c] = jnp.zeros_like(q)
        geo[3, c] = envelope
        geo[4, c] = inv
        geo[5, c] = (-4.0 / CUTOFF) * q * rest

    def ids_of(zr):
        return list(range(zr * cx, (zr + 1) * cx))

    def inner_of(zr):
        return ids_of(zr)[1:-1]

    def latents(rows):
        pres, lows, mls = {}, {}, {}
        for zr in rows:
            span = slice(zr * wide, (zr + 1) * wide)
            radial = join([rad[:, i, :] for i in ids_of(zr)], 1)
            rh = rounded(radial)
            x_s = xs[:, span]
            pres[zr] = dot(in_t, jnp.concatenate([
                jnp.concatenate([rh, radial - rh], axis=0).astype(BF16),
                jnp.concatenate([rh, jnp.zeros_like(rh)], axis=0).astype(BF16), x_s, x_s], axis=0))
        for zr in rows:
            span = slice(zr * wide, (zr + 1) * wide)
            pre = pres[zr]
            sig = 0.5 + 0.5 * jnp.tanh(0.5 * pre)
            latent = pre * sig
            dsilu[:, span] = sig + latent * (1.0 - sig)
            lh, ll = split(latent)
            if 1 <= zr <= bz:
                l2[zr - 1, 0] = lh[:, n : n + inner]
                l2[zr - 1, 1] = ll[:, n : n + inner]
            lows[zr] = dot(env_t2, jnp.concatenate([lh, ll], axis=0))
        for zr in rows:
            span = slice(zr * wide, (zr + 1) * wide)
            ids = ids_of(zr)
            w = lows[zr]
            w = (w[:ch] + w[ch:]) * join([rows_live[i : i + 1] for i in ids], 1)
            wts[:, span] = w
            msgs = jnp.concatenate(
                [w] + [w * join([harm[m, i : i + 1] for i in ids], 1) for m in range(3)], axis=0)
            mls[zr] = split(msgs)
            mh, ml = mls[zr]
            for t, i in enumerate(ids):
                cut = slice(t * n, (t + 1) * n)
                hot_c = hot_t[i, :, :n]
                feat[:, i * n : (i + 1) * n] = dot(
                    jnp.concatenate([mh[:, cut], ml[:, cut]], axis=1),
                    jnp.concatenate([hot_c, hot_c], axis=0)).astype(BF16)

    early, late = list(range(2, cz)), [0, 1]
    for k, ref in enumerate((atoms, edges)):
        received = ref.at[pl.ds(0, len(others_list))]
        whole(received, recv_sem.at[k])
        whole(received, send_sem.at[k])
    every = list(range(cz))
    decode(every)
    tables(range(bz - 2, 2 * bz + 2))
    for i in range(total):
        gather(i)
    geometry(every)
    latents(every)

    row_16 = lax.broadcasted_iota(jnp.int32, (16, n), 0)
    out_rows = jnp.concatenate([out_col] * bx, axis=1)
    inner_rows = range(1, bz + 1)
    f_cs, f_os, us, joins, raws = {}, {}, {}, {}, {}
    for zr in inner_rows:
        f_cs[zr] = join([dot(feat[:, i * n : (i + 1) * n], hot[i, :, :n]) for i in inner_of(zr)], 1)
        f_os[zr] = dot(feat[:, (zr - 1) * wide : (zr + 2) * wide], rows_hot[zr - 1])
    for zr in inner_rows:
        prod4 = f_cs[zr] * f_os[zr]
        prod = prod4[:ch] + prod4[ch : 2 * ch] + prod4[2 * ch : 3 * ch] + prod4[3 * ch :]
        ph, pl_ = split(prod)
        parts = [l2[zr - 1, 0], l2[zr - 1, 1], l2[zr - 1, 0], ph, pl_, ph]
        if kpad:
            parts.append(jnp.zeros((kpad, inner), BF16))
        us[zr] = dot(up_t, jnp.concatenate(parts, axis=0))
    for zr in inner_rows:
        env_row = join([geo[3, i : i + 1] for i in inner_of(zr)], 1)
        alive = join([rows_live[i : i + 1] for i in inner_of(zr)], 1)
        u = us[zr]
        sig = 0.5 + 0.5 * jnp.tanh(0.5 * u)
        hid = u * sig
        raws[zr] = jnp.sum(out_rows * hid, axis=0, keepdims=True) * alive
        d_u = out_rows * (alive * env_row) * (sig + hid * (1.0 - sig))
        dh, dl = split(d_u)
        joins[zr] = dot(up3, jnp.concatenate([dh, dl, dh], axis=0))
    for zr in inner_rows:
        d_join = joins[zr]
        dlat_own[zr - 1] = d_join[:lat]
        d_prod = jnp.concatenate([d_join[lat:]] * 4, axis=0)
        dch, dcl = split(d_prod * f_os[zr])
        doh, dol = split(d_prod * f_cs[zr])
        turned_rows = rows_hot_t[zr - 1]
        part = dot(jnp.concatenate([doh, dol], axis=1), jnp.concatenate([turned_rows, turned_rows], axis=0))
        if zr == 1:
            dfeat[:, : 3 * wide] = part
            if cz > 3:
                dfeat[:, 3 * wide :] = jnp.zeros((4 * ch, (cz - 3) * wide), F32)
        else:
            dfeat[:, (zr - 1) * wide : (zr + 2) * wide] += part
        for t, i in enumerate(inner_of(zr)):
            raw = raws[zr][:, t * n : (t + 1) * n]
            env_grad[i : i + 1] = raw
            e_row = raw * geo[3, i : i + 1]
            e_hi = rounded(e_row)
            e_lo = jnp.where(row_16 == 0, e_row - e_hi, 0.0).astype(BF16)
            e_hi = jnp.where(row_16 == 0, e_hi, 0.0).astype(BF16)
            cut = slice(t * n, (t + 1) * n)
            hot_c = hot_t[i, :, :n]
            both = dot(
                jnp.concatenate([
                    jnp.concatenate([dch[:, cut], e_hi], axis=0),
                    jnp.concatenate([dcl[:, cut], e_lo], axis=0)], axis=1),
                jnp.concatenate([hot_c, hot_c], axis=0))
            dfeat[:, i * n : (i + 1) * n] += both[: 4 * ch]
            grad[centre, zr - 1, t, 3:4] = -both[4 * ch : 4 * ch + 1]

    def backward(rows):
        dms, dls = {}, {}
        for zr in rows:
            dm = []
            for i in ids_of(zr):
                hot_c = hot[i, :, :n]
                fh, fl = split(dfeat[:, i * n : (i + 1) * n])
                dm.append(dot(jnp.concatenate([fh, fl], axis=1), jnp.concatenate([hot_c, hot_c], axis=0)))
            dms[zr] = join(dm, 1)
        for zr in rows:
            ids = ids_of(zr)
            dm = dms[zr]
            dw = dm[:ch]
            for m in range(3):
                dw = dw + dm[(m + 1) * ch : (m + 2) * ch] * join([harm[m, i : i + 1] for i in ids], 1)
            dw = dw * join([rows_live[i : i + 1] for i in ids], 1)
            wh, wl = split(dw)
            parts = [wh, wl, wh]
            if kpad:
                parts.append(jnp.zeros((kpad, wide), BF16))
            dls[zr] = dot(env3, jnp.concatenate(parts, axis=0))
        for zr in rows:
            span = slice(zr * wide, (zr + 1) * wide)
            d_lat = dls[zr]
            if 1 <= zr <= bz:
                side = jnp.zeros((lat, n), F32)
                d_lat = d_lat + jnp.concatenate([side, dlat_own[zr - 1], side], axis=1)
            dh, dl = split(d_lat * dsilu[:, span])
            d_r = dot(wr2, jnp.concatenate([dh, dl], axis=0))
            d_r = d_r[:nb] + d_r[nb:]
            for t, i in enumerate(ids_of(zr)):
                drad[:, i, :] = d_r[:, t * n : (t + 1) * n]
        for zr in rows:
            span = slice(zr * wide, (zr + 1) * wide)
            w = wts[:, span]
            for m in range(3):
                d_h = jnp.sum(dms[zr][(m + 1) * ch : (m + 2) * ch] * w, axis=0, keepdims=True)
                for t, i in enumerate(ids_of(zr)):
                    dharm[m, i : i + 1] = d_h[:, t * n : (t + 1) * n]

    def radial_backward(rows):
        c = slice(rows[0] * cx, (rows[-1] + 1) * cx)
        sum_s = drad[0, c] * sins[0, c]
        sum_c = drad[0, c] * coss[0, c]
        for k in range(1, nb):
            sum_s = sum_s + drad[k, c] * sins[k, c]
            sum_c = sum_c + (k + 1.0) * (drad[k, c] * coss[k, c])
        inv, env_slope = geo[4, c], geo[5, c]
        scale = inv * geo[3, c]
        d_dist = (
            (math.pi / CUTOFF) * sum_c * scale
            - sum_s * scale * inv
            + (sum_s * inv + env_grad[c]) * env_slope
        )
        for m in range(3):
            d_dist = d_dist - dharm[m, c] * geo[m, c] * (inv * inv)
        for m in range(3):
            d_m = d_dist * harm[m, c] + dharm[m, c] * inv
            hi = rounded(d_m)
            gr[c, m, :] = hi
            gr[c, m + 4, :] = d_m - hi
        gr[c, 3, :] = jnp.zeros_like(inv)
        gr[c, 7, :] = jnp.zeros_like(inv)

    def scatter(i):
        a, b = cells[i]
        g8 = gr[i]
        p = rows_p[i : i + 1]
        stack = [g8] + [jnp.where(p == off, g8, 0.0) for off in range(9)]
        out = dot(jnp.concatenate(stack, axis=0).astype(BF16), hot_t[i])
        s, y, x = place(a, b)
        grad[s, y, x] -= out[:8, :n]
        for off in range(9):
            s, y, x = place(a + off // 3 - 1, b + off % 3 - 1)
            grad[s, y, x] += out[8 + 8 * off : 16 + 8 * off, n:]

    second = {}

    def give(later):
        for key, s in others_list:
            if s in second or s in later:
                continue
            i = index[s]
            for y in range(bz):
                for x in range(bx):
                    acc = grad[s, y, x]
                    give_ref[i, y, x] = acc[:4] + acc[4:]
            second[s] = pltpu.make_async_remote_copy(
                src_ref=give_ref.at[i], dst_ref=back.at[i], send_sem=send_sem.at[2],
                recv_sem=recv_sem.at[2], device_id=owner(key), device_id_type=MESH,
            )
            second[s].start()

    def targets(rows):
        return {
            place(cells[i][0] + dz, cells[i][1] + dx)[0]
            for zr in rows for i in ids_of(zr) for dz in (-1, 0, 1) for dx in (-1, 0, 1)}

    backward(early[::-1])
    radial_backward(early)
    for zr in reversed(early):
        for i in ids_of(zr):
            scatter(i)
    give(targets(late))
    backward(late[::-1])
    radial_backward(late)
    for zr in reversed(late):
        for i in ids_of(zr):
            scatter(i)
    give(set())
    whole(give_ref, send_sem.at[2])
    whole(back, recv_sem.at[2])
    for a in range(bz):
        for b in range(bx):
            acc = grad[mine, a, b]
            acc = acc[:4] + acc[4:]
            for s in range(len(others_list)):
                acc = acc + back[s, a, b]
            result_ref[:, a, b, :] = -acc


def deliver(result_ref, energy_ref, force_ref, sem):
    copies = [
        pltpu.make_async_copy(result_ref.at[3], energy_ref, sem.at[0]),
        pltpu.make_async_copy(result_ref.at[pl.ds(0, 3)], force_ref, sem.at[1]),
    ]
    for copy in copies:
        copy.start()
    for copy in copies:
        copy.wait()


def solution(mesh):
    nz, nx = mesh.shape["gz"], mesh.shape["xy"]

    def body(coords, species, centers, others, live_count, in_weight, env_weight, up_weight, out_weight):
        _, bz, bx, n = coords.shape
        lat, ch = env_weight.shape
        nb = 8
        spec = (in_weight.shape[0] - nb) // 2
        cells = (bz + 2) * (bx + 2)
        ns = len(neighbours(nz, nx)) - 1
        vmem = lambda shape, dtype=F32: pltpu.VMEM(shape, dtype)
        args = (coords, species, centers, others, live_count, in_weight, env_weight.T, up_weight,
                out_weight[None])
        scratch = [
            vmem(coords.shape),
            vmem((3, bz, bx, n), jnp.int32),
            vmem((bz, bx), jnp.int32),
            vmem((sum(w.shape[0] for w in args[5:8]), lat)),
            vmem((1, lat)),
            vmem((ns + 1, bz, bx, 4, n)),
            vmem((ns + 1, bz, bx, n)),
            vmem((3 * bz, 3 * bx, 32, n), BF16),
            vmem((cells, n, 2 * n), BF16),
            vmem((cells, n, 2 * n), BF16),
            vmem((bz, 3 * (bx + 2) * n, bx * n), BF16),
            vmem((bz, bx * n, 3 * (bx + 2) * n), BF16),
            vmem((cells, n)),
            vmem((cells, n)),
            vmem((cells, n)),
            vmem((cells, n), jnp.int32),
            vmem((cells, n)),
            vmem((cells, 4, n)),
            vmem((6, cells, n)),
            vmem((2 * spec, cells * n), BF16),
            vmem((nb, cells, n)),
            vmem((nb, cells, n)),
            vmem((nb, cells, n)),
            vmem((3, cells, n)),
            vmem((bz, 2, lat, bx * n), BF16),
            vmem((lat, cells * n)),
            vmem((ch, cells * n)),
            vmem((4 * ch, cells * n), BF16),
            vmem((4 * ch, cells * n)),
            vmem((bz, lat, bx * n)),
            vmem((cells, n)),
            vmem((3, cells, n)),
            vmem((nb, cells, n)),
            vmem((cells, 8, n)),
            vmem((ns + 1, bz, bx, 8, n)),
            vmem((ns, bz, bx, 4, n)),
            vmem((ns, bz, bx, 4, n)),
            pltpu.SemaphoreType.DMA((3,)),
            pltpu.SemaphoreType.DMA((3,)),
            pltpu.SemaphoreType.DMA((5,)),
        ]
        specs = [pl.BlockSpec(memory_space=pl.ANY) for _ in args]
        result = pl.pallas_call(
            functools.partial(kernel, nz, nx, bz, bx, nb, spec, ch, lat),
            out_shape=pltpu.VMEM((4, bz, bx, n), F32),
            in_specs=specs,
            out_specs=pl.BlockSpec(memory_space=pltpu.VMEM),
            scratch_shapes=scratch,
            compiler_params=pltpu.CompilerParams(collective_id=0, has_side_effects=True),
        )(*args)
        return pl.pallas_call(
            deliver,
            out_shape=(jax.ShapeDtypeStruct((bz, bx, n), F32), jax.ShapeDtypeStruct((3, bz, bx, n), F32)),
            in_specs=[pl.BlockSpec(memory_space=pltpu.VMEM)],
            out_specs=(pl.BlockSpec(memory_space=pl.ANY), pl.BlockSpec(memory_space=pl.ANY)),
            scratch_shapes=[pltpu.SemaphoreType.DMA((2,))],
        )(pltpu.with_memory_space_constraint(result, pltpu.VMEM))

    in_specs = (
        P(None, "gz", "xy", None), P("gz", "xy", None), P("gz", "xy", None), P("gz", "xy", None),
        P("gz", "xy"), P(), P(), P(), P(),
    )
    out_specs = (P("gz", "xy", None), P(None, "gz", "xy", None))
    return jax.shard_map(body, mesh=mesh, in_specs=in_specs, out_specs=out_specs, check_vma=False)
```

```python
import functools
import math

import jax
import jax.numpy as jnp
from jax import lax
from jax.experimental import pallas as pl
from jax.experimental.pallas import tpu as pltpu
from jax.sharding import PartitionSpec as P

SOFTEN = 0.01
CUTOFF = 3.5
F32 = jnp.float32
BF16 = jnp.bfloat16
MESH = pl.DeviceIdType.MESH


def rounded(x):
    return x.astype(BF16).astype(F32)


def split(x):
    high = x.astype(BF16)
    return high, (x - high.astype(F32)).astype(BF16)


def dot(a, b):
    return jnp.dot(a, b, preferred_element_type=F32)


def dot_t(a, b):
    return lax.dot_general(a, b, (((1,), (1,)), ((), ())), preferred_element_type=F32)


def join(parts, axis):
    return parts[0] if len(parts) == 1 else jnp.concatenate(parts, axis=axis)


def neighbours(nz, nx):
    slots = {(0, 0): 0}
    for dz in (-1, 0, 1):
        for dx in (-1, 0, 1):
            slots.setdefault((dz % nz, dx % nx), len(slots))
    return slots


def kernel(
    nz, nx, bz, bx, nb, spec, ch, lat,
    coords_hbm, species_hbm, centers_hbm, others_hbm, live_hbm, in_hbm, env_hbm, up_hbm, out_hbm,
    result_ref,
    coords_ref, ints_ref, live_ref, weights_ref, out_ref,
    atoms, edges, tab, hot, hot_t, rows_hot, rows_hot_t, codes, rows_c, rows_o, rows_p, rows_live,
    diffs, geo, xs, sins, coss, rad, harm,
    l2, dsilu, wts, feat, dfeat, dlat_own, env_grad, dharm, drad, gr, grad, give_ref, back,
    send_sem, recv_sem, load_sem,
):
    n = coords_ref.shape[-1]
    slots = neighbours(nz, nx)
    me_z, me_x = lax.axis_index("gz"), lax.axis_index("xy")
    mine = slots[(1 % nz, 0)]
    last = len(slots) - 1
    slots = {key: last if s == mine else mine if s == last else s for key, s in slots.items()}
    mine = last
    centre = slots[(0, 0)]
    others_list = [(key, s) for key, s in slots.items() if s != mine]
    index = {s: i for i, (_, s) in enumerate(others_list)}

    def owner(key):
        return (lax.rem(me_z + (key[0] - 1) % nz, nz), lax.rem(me_x + key[1], nx))

    def user(key):
        return (lax.rem(me_z + (1 - key[0]) % nz, nz), lax.rem(me_x + (-key[1]) % nx, nx))

    barrier = pltpu.get_barrier_semaphore()
    for key, _ in others_list:
        pl.semaphore_signal(barrier, inc=1, device_id=owner(key), device_id_type=MESH)

    def whole(ref, sem):
        pltpu.make_async_copy(ref, ref, sem).wait()

    for k, (source, target) in enumerate([
            (coords_hbm, coords_ref), (live_hbm, live_ref), (out_hbm, out_ref)]):
        pltpu.make_async_copy(source, target, load_sem.at[k]).start()
    for k, source in enumerate((species_hbm, centers_hbm, others_hbm)):
        pltpu.make_async_copy(source, ints_ref.at[k], load_sem.at[3]).start()
    rows_in, rows_env, rows_up = in_hbm.shape[0], env_hbm.shape[0], up_hbm.shape[0]
    row = 0
    for source in (in_hbm, env_hbm, up_hbm):
        pltpu.make_async_copy(source, weights_ref.at[pl.ds(row, source.shape[0])], load_sem.at[4]).start()
        row += source.shape[0]
    whole(coords_ref, load_sem.at[0])
    whole(live_ref, load_sem.at[1])
    whole(ints_ref, load_sem.at[3])
    lane = lax.broadcasted_iota(jnp.int32, (1, n), 1)
    for a in range(bz):
        for b in range(bx):
            code = ints_ref[1, a, b : b + 1, :] + 128 * ints_ref[2, a, b : b + 1, :]
            code = jnp.where(lane < live_ref[a : a + 1, b : b + 1], code, -1)
            edges[mine, a, b : b + 1, :] = code.astype(F32)
            atoms[mine, a, b] = jnp.concatenate(
                [coords_ref[:, a, b, :], ints_ref[0, a, b : b + 1, :].astype(F32)], axis=0)
    pl.semaphore_wait(barrier, len(others_list))
    for key, s in others_list:
        for k, ref in enumerate((atoms, edges)):
            pltpu.make_async_remote_copy(
                src_ref=ref.at[mine], dst_ref=ref.at[s], send_sem=send_sem.at[k],
                recv_sem=recv_sem.at[k], device_id=user(key), device_id_type=MESH,
            ).start()

    whole(out_ref, load_sem.at[2])
    whole(weights_ref, load_sem.at[4])
    w_in = weights_ref[:rows_in]
    w_hi = rounded(w_in)
    w_lo = w_in - w_hi
    gap = jnp.zeros((nb, lat), F32)
    kin = 4 * nb + 4 * spec
    w_rows = [w_hi[:nb], w_hi[:nb], w_lo[:nb], gap, w_hi[nb:], w_lo[nb:]]
    if lat > kin:
        w_rows.append(jnp.zeros((lat - kin, lat), F32))
    in_t = jnp.concatenate(w_rows, axis=0).T.astype(BF16)[:, :kin]
    wr2 = jnp.concatenate(
        [jnp.concatenate([w_hi[:nb], w_hi[:nb]], axis=1), jnp.concatenate([w_lo[:nb], gap], axis=1)],
        axis=0).astype(BF16)
    env_t = weights_ref[rows_in : rows_in + rows_env]
    et_hi = rounded(env_t)
    et_lo = env_t - et_hi
    env_t2 = jnp.concatenate(
        [jnp.concatenate([et_hi, et_hi], axis=1), jnp.concatenate([et_lo, jnp.zeros_like(et_lo)], axis=1)],
        axis=0).astype(BF16)
    kpad = -(3 * ch) % lat
    env3 = jnp.concatenate(
        [et_hi, et_hi, et_lo] + ([jnp.zeros((kpad, lat), F32)] if kpad else []), axis=0
    ).T.astype(BF16)
    up = weights_ref[rows_in + rows_env :]
    up_hi = rounded(up)
    up_lo = up - up_hi
    up3 = jnp.concatenate([up_hi, up_hi, up_lo], axis=1).astype(BF16)
    up_t = jnp.concatenate(
        [x.T.astype(BF16) for x in (up_hi[:lat], up_hi[:lat], up_lo[:lat])]
        + [jnp.concatenate(
            [up_hi[lat:], up_hi[lat:], up_lo[lat:]]
            + ([jnp.zeros((kpad, lat), F32)] if kpad else []), axis=0).T.astype(BF16)],
        axis=1)
    out_col = jnp.broadcast_to(out_ref[...], (n, lat)).T

    rows_hot[...] = jnp.zeros_like(rows_hot)
    rows_hot_t[...] = jnp.zeros_like(rows_hot_t)
    grad[...] = jnp.zeros_like(grad)
    cz, cx = bz + 2, bx + 2
    total = cz * cx
    wide = cx * n
    inner = bx * n
    cells = [(a, b) for a in range(bz - 1, 2 * bz + 1) for b in range(bx - 1, 2 * bx + 1)]
    row_n = lax.broadcasted_iota(jnp.int32, (n, n), 0).astype(F32).astype(BF16)
    row_s = lax.broadcasted_iota(jnp.int32, (spec, n), 0).astype(F32)
    one, zero = jnp.ones((n, n), BF16), jnp.zeros((n, n), BF16)

    def place(a, b):
        return slots[((a // bz - 1) % nz, (b // bx - 1) % nx)], a % bz, b % bx

    def tables(rows):
        for a in rows:
            hl = {}
            for b in range(bx - 2, 2 * bx + 2):
                s, i, j = place(a, b)
                part = atoms[s, i, j]
                hi = rounded(part)
                hl[b] = jnp.concatenate([hi, part - hi], axis=0)
            for b in range(bx - 1, 2 * bx + 1):
                tab[a, b] = jnp.concatenate(
                    [hl[b - 1], hl[b], hl[b + 1], jnp.zeros((8, n), F32)], axis=0).astype(BF16)

    def decode(rows):
        c = slice(rows[0] * cx, (rows[-1] + 1) * cx)
        for i in range(rows[0] * cx, (rows[-1] + 1) * cx):
            s, y, x = place(*cells[i])
            codes[i : i + 1] = edges[s, y, x : x + 1, :]
        code = codes[c].astype(jnp.int32)
        o = code >> 7
        rows_c[c] = (code & 127).astype(F32)
        rows_o[c] = (o & 127).astype(F32)
        rows_p[c] = o >> 7
        rows_live[c] = (code >= 0).astype(F32)

    def gather(i):
        a, b = cells[i]
        p = rows_p[i : i + 1]
        hot_c = jnp.where(row_n == rows_c[i : i + 1].astype(BF16), one, zero)
        hot_o = jnp.where(row_n == rows_o[i : i + 1].astype(BF16), one, zero)
        both = jnp.concatenate([hot_c, hot_o], axis=1)
        hot[i] = both
        hot_t[i] = jnp.concatenate([hot_c.T, hot_o.T], axis=1)
        zr, xc = i // cx, i % cx
        if 1 <= zr <= bz and 1 <= xc <= bx:
            for dz in range(3):
                for dx in range(3):
                    col = dz * cx + xc - 1 + dx
                    masked = hot_o * (p == 3 * dz + dx).astype(F32).astype(BF16)
                    rows_hot[zr - 1, col * n : (col + 1) * n, (xc - 1) * n : xc * n] = masked
                    rows_hot_t[zr - 1, (xc - 1) * n : xc * n, col * n : (col + 1) * n] = masked.T
        around = jnp.concatenate([tab[a + dz, b] for dz in (-1, 0, 1)], axis=0)
        got = dot(around, both)
        at_c = got[40:48, :n]
        at_o = jnp.zeros((8, n), F32)
        for dz in range(3):
            for dx in range(3):
                at_o = jnp.where(p == 3 * dz + dx, got[32 * dz + 8 * dx : 32 * dz + 8 * dx + 8, n:], at_o)
        at_c = at_c[:4] + at_c[4:]
        at_o = at_o[:4] + at_o[4:]
        diffs[i] = at_o - at_c
        xs[:, i * n : (i + 1) * n] = jnp.concatenate(
            [(row_s == at_c[3:4]).astype(F32), (row_s == at_o[3:4]).astype(F32)], axis=0).astype(BF16)

    def geometry(rows):
        c = slice(rows[0] * cx, (rows[-1] + 1) * cx)
        p = rows_p[c]
        third = (p >= 3).astype(jnp.int32) + (p >= 6).astype(jnp.int32)
        r = [
            diffs[c, 0, :] + (third - 1).astype(F32),
            diffs[c, 1, :] + (p - 3 * third - 1).astype(F32),
            diffs[c, 2, :],
        ]
        dist = jnp.sqrt(r[0] * r[0] + r[1] * r[1] + r[2] * r[2] + SOFTEN)
        inv = 1.0 / dist
        q = dist / CUTOFF
        rest = 1.0 - q * q
        envelope = rest * rest
        scale = inv * envelope
        t1 = math.pi * (q - 0.5)
        t2 = t1 * t1
        s1, c1 = jnp.ones_like(q), jnp.ones_like(q)
        for m in range(7, 0, -1):
            s1 = 1.0 - t2 * s1 * (1.0 / ((2 * m - 1) * (2 * m)))
            c1 = 1.0 - t2 * c1 * (1.0 / ((2 * m) * (2 * m + 1)))
        c1 = -t1 * c1
        s0, c0, sk, ck = jnp.zeros_like(s1), jnp.ones_like(c1), s1, c1
        for k in range(nb):
            sins[k, c] = sk
            coss[k, c] = ck
            rad[k, c] = sk * scale
            s0, sk = sk, 2.0 * c1 * sk - s0
            c0, ck = ck, 2.0 * c1 * ck - c0
        for m in range(3):
            harm[m, c] = r[m] * inv
            geo[m, c] = r[m]
        env_grad[c] = jnp.zeros_like(q)
        geo[3, c] = envelope
        geo[4, c] = inv
        geo[5, c] = (-4.0 / CUTOFF) * q * rest

    def ids_of(zr):
        return list(range(zr * cx, (zr + 1) * cx))

    def inner_of(zr):
        return ids_of(zr)[1:-1]

    def latents(rows):
        pres, lows, mls = {}, {}, {}
        for zr in rows:
            span = slice(zr * wide, (zr + 1) * wide)
            radial = join([rad[:, i, :] for i in ids_of(zr)], 1)
            rh = rounded(radial)
            x_s = xs[:, span]
            pres[zr] = dot(in_t, jnp.concatenate([
                jnp.concatenate([rh, radial - rh], axis=0).astype(BF16),
                jnp.concatenate([rh, jnp.zeros_like(rh)], axis=0).astype(BF16), x_s, x_s], axis=0))
        for zr in rows:
            span = slice(zr * wide, (zr + 1) * wide)
            pre = pres[zr]
            sig = 0.5 + 0.5 * jnp.tanh(0.5 * pre)
            latent = pre * sig
            dsilu[:, span] = sig + latent * (1.0 - sig)
            lh, ll = split(latent)
            if 1 <= zr <= bz:
                l2[zr - 1, 0] = lh[:, n : n + inner]
                l2[zr - 1, 1] = ll[:, n : n + inner]
            lows[zr] = dot(env_t2, jnp.concatenate([lh, ll], axis=0))
        for zr in rows:
            span = slice(zr * wide, (zr + 1) * wide)
            ids = ids_of(zr)
            w = lows[zr]
            w = (w[:ch] + w[ch:]) * join([rows_live[i : i + 1] for i in ids], 1)
            wts[:, span] = w
            msgs = jnp.concatenate(
                [w] + [w * join([harm[m, i : i + 1] for i in ids], 1) for m in range(3)], axis=0)
            mls[zr] = split(msgs)
            mh, ml = mls[zr]
            for t, i in enumerate(ids):
                cut = slice(t * n, (t + 1) * n)
                hot_c = hot_t[i, :, :n]
                feat[:, i * n : (i + 1) * n] = dot(
                    jnp.concatenate([mh[:, cut], ml[:, cut]], axis=1),
                    jnp.concatenate([hot_c, hot_c], axis=0)).astype(BF16)

    early, late = list(range(2, cz)), [0, 1]
    for k, ref in enumerate((atoms, edges)):
        received = ref.at[pl.ds(0, len(others_list))]
        whole(received, recv_sem.at[k])
        whole(received, send_sem.at[k])
    every = list(range(cz))
    decode(every)
    tables(range(bz - 2, 2 * bz + 2))
    for i in range(total):
        gather(i)
    geometry(every)
    latents(every)

    row_16 = lax.broadcasted_iota(jnp.int32, (16, n), 0)
    out_rows = jnp.concatenate([out_col] * bx, axis=1)
    inner_rows = range(1, bz + 1)
    f_cs, f_os, us, joins, raws = {}, {}, {}, {}, {}
    for zr in inner_rows:
        f_cs[zr] = join([dot(feat[:, i * n : (i + 1) * n], hot[i, :, :n]) for i in inner_of(zr)], 1)
        f_os[zr] = dot(feat[:, (zr - 1) * wide : (zr + 2) * wide], rows_hot[zr - 1])
    for zr in inner_rows:
        prod4 = f_cs[zr] * f_os[zr]
        prod = prod4[:ch] + prod4[ch : 2 * ch] + prod4[2 * ch : 3 * ch] + prod4[3 * ch :]
        ph, pl_ = split(prod)
        parts = [l2[zr - 1, 0], l2[zr - 1, 1], l2[zr - 1, 0], ph, pl_, ph]
        if kpad:
            parts.append(jnp.zeros((kpad, inner), BF16))
        us[zr] = dot(up_t, jnp.concatenate(parts, axis=0))
    for zr in inner_rows:
        env_row = join([geo[3, i : i + 1] for i in inner_of(zr)], 1)
        alive = join([rows_live[i : i + 1] for i in inner_of(zr)], 1)
        u = us[zr]
        sig = 0.5 + 0.5 * jnp.tanh(0.5 * u)
        hid = u * sig
        raws[zr] = jnp.sum(out_rows * hid, axis=0, keepdims=True) * alive
        d_u = out_rows * (alive * env_row) * (sig + hid * (1.0 - sig))
        dh, dl = split(d_u)
        joins[zr] = dot(up3, jnp.concatenate([dh, dl, dh], axis=0))
    dcs, dos = {}, {}
    for zr in inner_rows:
        d_join = joins[zr]
        dlat_own[zr - 1] = d_join[:lat]
        d_prod = jnp.concatenate([d_join[lat:]] * 4, axis=0)
        dcs[zr] = split(d_prod * f_os[zr])
        dos[zr] = jnp.concatenate(split(d_prod * f_cs[zr]), axis=1)

    def feature_gradient(rows):
        for r in rows:
            acc = None
            for zr in inner_rows:
                if abs(r - zr) <= 1:
                    at = r - zr + 1
                    block = rows_hot_t[zr - 1, :, at * wide : (at + 1) * wide]
                    term = dot(dos[zr], jnp.concatenate([block, block], axis=0))
                    acc = term if acc is None else acc + term
            if r in inner_rows:
                side = jnp.zeros((4 * ch, n), F32)
                tops = [side]
                for t, i in enumerate(inner_of(r)):
                    cut = slice(t * n, (t + 1) * n)
                    raw = raws[r][:, cut]
                    env_grad[i : i + 1] = raw
                    e_row = raw * geo[3, i : i + 1]
                    e_hi = rounded(e_row)
                    e_lo = jnp.where(row_16 == 0, e_row - e_hi, 0.0).astype(BF16)
                    e_hi = jnp.where(row_16 == 0, e_hi, 0.0).astype(BF16)
                    hot_c = hot_t[i, :, :n]
                    dch, dcl = dcs[r]
                    both = dot(
                        jnp.concatenate([
                            jnp.concatenate([dch[:, cut], e_hi], axis=0),
                            jnp.concatenate([dcl[:, cut], e_lo], axis=0)], axis=1),
                        jnp.concatenate([hot_c, hot_c], axis=0))
                    tops.append(both[: 4 * ch])
                    grad[centre, r - 1, t, 3:4] = -both[4 * ch : 4 * ch + 1]
                acc = acc + jnp.concatenate(tops + [side], axis=1)
            dfeat[:, r * wide : (r + 1) * wide] = acc

    def backward(rows):
        dms, dls = {}, {}
        for zr in rows:
            dm = []
            for i in ids_of(zr):
                hot_c = hot[i, :, :n]
                fh, fl = split(dfeat[:, i * n : (i + 1) * n])
                dm.append(dot(jnp.concatenate([fh, fl], axis=1), jnp.concatenate([hot_c, hot_c], axis=0)))
            dms[zr] = join(dm, 1)
        for zr in rows:
            ids = ids_of(zr)
            dm = dms[zr]
            dw = dm[:ch]
            for m in range(3):
                dw = dw + dm[(m + 1) * ch : (m + 2) * ch] * join([harm[m, i : i + 1] for i in ids], 1)
            dw = dw * join([rows_live[i : i + 1] for i in ids], 1)
            wh, wl = split(dw)
            parts = [wh, wl, wh]
            if kpad:
                parts.append(jnp.zeros((kpad, wide), BF16))
            dls[zr] = dot(env3, jnp.concatenate(parts, axis=0))
        for zr in rows:
            span = slice(zr * wide, (zr + 1) * wide)
            d_lat = dls[zr]
            if 1 <= zr <= bz:
                side = jnp.zeros((lat, n), F32)
                d_lat = d_lat + jnp.concatenate([side, dlat_own[zr - 1], side], axis=1)
            dh, dl = split(d_lat * dsilu[:, span])
            d_r = dot(wr2, jnp.concatenate([dh, dl], axis=0))
            d_r = d_r[:nb] + d_r[nb:]
            for t, i in enumerate(ids_of(zr)):
                drad[:, i, :] = d_r[:, t * n : (t + 1) * n]
        for zr in rows:
            span = slice(zr * wide, (zr + 1) * wide)
            w = wts[:, span]
            for m in range(3):
                d_h = jnp.sum(dms[zr][(m + 1) * ch : (m + 2) * ch] * w, axis=0, keepdims=True)
                for t, i in enumerate(ids_of(zr)):
                    dharm[m, i : i + 1] = d_h[:, t * n : (t + 1) * n]

    def radial_backward(rows):
        c = slice(rows[0] * cx, (rows[-1] + 1) * cx)
        sum_s = drad[0, c] * sins[0, c]
        sum_c = drad[0, c] * coss[0, c]
        for k in range(1, nb):
            sum_s = sum_s + drad[k, c] * sins[k, c]
            sum_c = sum_c + (k + 1.0) * (drad[k, c] * coss[k, c])
        inv, env_slope = geo[4, c], geo[5, c]
        scale = inv * geo[3, c]
        d_dist = (
            (math.pi / CUTOFF) * sum_c * scale
            - sum_s * scale * inv
            + (sum_s * inv + env_grad[c]) * env_slope
        )
        for m in range(3):
            d_dist = d_dist - dharm[m, c] * geo[m, c] * (inv * inv)
        for m in range(3):
            d_m = d_dist * harm[m, c] + dharm[m, c] * inv
            hi = rounded(d_m)
            gr[c, m, :] = hi
            gr[c, m + 4, :] = d_m - hi
        gr[c, 3, :] = jnp.zeros_like(inv)
        gr[c, 7, :] = jnp.zeros_like(inv)

    def scatter(i):
        a, b = cells[i]
        g8 = gr[i]
        p = rows_p[i : i + 1]
        stack = [g8] + [jnp.where(p == off, g8, 0.0) for off in range(9)]
        out = dot(jnp.concatenate(stack, axis=0).astype(BF16), hot_t[i])
        s, y, x = place(a, b)
        grad[s, y, x] -= out[:8, :n]
        for off in range(9):
            s, y, x = place(a + off // 3 - 1, b + off % 3 - 1)
            grad[s, y, x] += out[8 + 8 * off : 16 + 8 * off, n:]

    second = {}

    def give(later):
        for key, s in others_list:
            if s in second or s in later:
                continue
            i = index[s]
            for y in range(bz):
                for x in range(bx):
                    acc = grad[s, y, x]
                    give_ref[i, y, x] = acc[:4] + acc[4:]
            second[s] = pltpu.make_async_remote_copy(
                src_ref=give_ref.at[i], dst_ref=back.at[i], send_sem=send_sem.at[2],
                recv_sem=recv_sem.at[2], device_id=owner(key), device_id_type=MESH,
            )
            second[s].start()

    def targets(rows):
        return {
            place(cells[i][0] + dz, cells[i][1] + dx)[0]
            for zr in rows for i in ids_of(zr) for dz in (-1, 0, 1) for dx in (-1, 0, 1)}

    feature_gradient(early)
    backward(early[::-1])
    radial_backward(early)
    for zr in reversed(early):
        for i in ids_of(zr):
            scatter(i)
    give(targets(late))
    feature_gradient(late)
    backward(late[::-1])
    radial_backward(late)
    for zr in reversed(late):
        for i in ids_of(zr):
            scatter(i)
    give(set())
    whole(give_ref, send_sem.at[2])
    whole(back, recv_sem.at[2])
    for a in range(bz):
        for b in range(bx):
            acc = grad[mine, a, b]
            acc = acc[:4] + acc[4:]
            for s in range(len(others_list)):
                acc = acc + back[s, a, b]
            result_ref[:, a, b, :] = -acc


def deliver(result_ref, energy_ref, force_ref, sem):
    copies = [
        pltpu.make_async_copy(result_ref.at[3], energy_ref, sem.at[0]),
        pltpu.make_async_copy(result_ref.at[pl.ds(0, 3)], force_ref, sem.at[1]),
    ]
    for copy in copies:
        copy.start()
    for copy in copies:
        copy.wait()


def solution(mesh):
    nz, nx = mesh.shape["gz"], mesh.shape["xy"]

    def body(coords, species, centers, others, live_count, in_weight, env_weight, up_weight, out_weight):
        _, bz, bx, n = coords.shape
        lat, ch = env_weight.shape
        nb = 8
        spec = (in_weight.shape[0] - nb) // 2
        cells = (bz + 2) * (bx + 2)
        ns = len(neighbours(nz, nx)) - 1
        vmem = lambda shape, dtype=F32: pltpu.VMEM(shape, dtype)
        args = (coords, species, centers, others, live_count, in_weight, env_weight.T, up_weight,
                out_weight[None])
        scratch = [
            vmem(coords.shape),
            vmem((3, bz, bx, n), jnp.int32),
            vmem((bz, bx), jnp.int32),
            vmem((sum(w.shape[0] for w in args[5:8]), lat)),
            vmem((1, lat)),
            vmem((ns + 1, bz, bx, 4, n)),
            vmem((ns + 1, bz, bx, n)),
            vmem((3 * bz, 3 * bx, 32, n), BF16),
            vmem((cells, n, 2 * n), BF16),
            vmem((cells, n, 2 * n), BF16),
            vmem((bz, 3 * (bx + 2) * n, bx * n), BF16),
            vmem((bz, bx * n, 3 * (bx + 2) * n), BF16),
            vmem((cells, n)),
            vmem((cells, n)),
            vmem((cells, n)),
            vmem((cells, n), jnp.int32),
            vmem((cells, n)),
            vmem((cells, 4, n)),
            vmem((6, cells, n)),
            vmem((2 * spec, cells * n), BF16),
            vmem((nb, cells, n)),
            vmem((nb, cells, n)),
            vmem((nb, cells, n)),
            vmem((3, cells, n)),
            vmem((bz, 2, lat, bx * n), BF16),
            vmem((lat, cells * n)),
            vmem((ch, cells * n)),
            vmem((4 * ch, cells * n), BF16),
            vmem((4 * ch, cells * n)),
            vmem((bz, lat, bx * n)),
            vmem((cells, n)),
            vmem((3, cells, n)),
            vmem((nb, cells, n)),
            vmem((cells, 8, n)),
            vmem((ns + 1, bz, bx, 8, n)),
            vmem((ns, bz, bx, 4, n)),
            vmem((ns, bz, bx, 4, n)),
            pltpu.SemaphoreType.DMA((3,)),
            pltpu.SemaphoreType.DMA((3,)),
            pltpu.SemaphoreType.DMA((5,)),
        ]
        specs = [pl.BlockSpec(memory_space=pl.ANY) for _ in args]
        result = pl.pallas_call(
            functools.partial(kernel, nz, nx, bz, bx, nb, spec, ch, lat),
            out_shape=pltpu.VMEM((4, bz, bx, n), F32),
            in_specs=specs,
            out_specs=pl.BlockSpec(memory_space=pltpu.VMEM),
            scratch_shapes=scratch,
            compiler_params=pltpu.CompilerParams(collective_id=0, has_side_effects=True),
        )(*args)
        return pl.pallas_call(
            deliver,
            out_shape=(jax.ShapeDtypeStruct((bz, bx, n), F32), jax.ShapeDtypeStruct((3, bz, bx, n), F32)),
            in_specs=[pl.BlockSpec(memory_space=pltpu.VMEM)],
            out_specs=(pl.BlockSpec(memory_space=pl.ANY), pl.BlockSpec(memory_space=pl.ANY)),
            scratch_shapes=[pltpu.SemaphoreType.DMA((2,))],
        )(pltpu.with_memory_space_constraint(result, pltpu.VMEM))

    in_specs = (
        P(None, "gz", "xy", None), P("gz", "xy", None), P("gz", "xy", None), P("gz", "xy", None),
        P("gz", "xy"), P(), P(), P(), P(),
    )
    out_specs = (P("gz", "xy", None), P(None, "gz", "xy", None))
    return jax.shard_map(body, mesh=mesh, in_specs=in_specs, out_specs=out_specs, check_vma=False)
```

```python
import functools
import math

import jax
import jax.numpy as jnp
from jax import lax
from jax.experimental import pallas as pl
from jax.experimental.pallas import tpu as pltpu
from jax.sharding import PartitionSpec as P

SOFTEN = 0.01
CUTOFF = 3.5
F32 = jnp.float32
BF16 = jnp.bfloat16
MESH = pl.DeviceIdType.MESH


def rounded(x):
    return x.astype(BF16).astype(F32)


def split(x):
    high = x.astype(BF16)
    return high, (x - high.astype(F32)).astype(BF16)


def dot(a, b):
    return jnp.dot(a, b, preferred_element_type=F32)


def dot_t(a, b):
    return lax.dot_general(a, b, (((1,), (1,)), ((), ())), preferred_element_type=F32)


def join(parts, axis):
    return parts[0] if len(parts) == 1 else jnp.concatenate(parts, axis=axis)


def neighbours(nz, nx):
    slots = {(0, 0): 0}
    for dz in (-1, 0, 1):
        for dx in (-1, 0, 1):
            slots.setdefault((dz % nz, dx % nx), len(slots))
    return slots


def kernel(
    nz, nx, bz, bx, nb, spec, ch, lat,
    coords_hbm, species_hbm, centers_hbm, others_hbm, live_hbm, in_hbm, env_hbm, up_hbm, out_hbm,
    result_ref,
    coords_ref, ints_ref, live_ref, weights_ref, out_ref,
    atoms, edges, tab, hot, hot_t, rows_hot, rows_hot_t, codes, rows_c, rows_o, rows_p, rows_live,
    diffs, geo, xs, sins, coss, rad, harm,
    l2, sigs, lats, wts, feat, dfeat, dlat_own, env_grad, dharm, drad, gr, grad, give_ref, back,
    send_sem, recv_sem, load_sem,
):
    n = coords_ref.shape[-1]
    slots = neighbours(nz, nx)
    me_z, me_x = lax.axis_index("gz"), lax.axis_index("xy")
    mine = slots[(1 % nz, 0)]
    last = len(slots) - 1
    slots = {key: last if s == mine else mine if s == last else s for key, s in slots.items()}
    mine = last
    centre = slots[(0, 0)]
    others_list = [(key, s) for key, s in slots.items() if s != mine]
    index = {s: i for i, (_, s) in enumerate(others_list)}

    def owner(key):
        return (lax.rem(me_z + (key[0] - 1) % nz, nz), lax.rem(me_x + key[1], nx))

    def user(key):
        return (lax.rem(me_z + (1 - key[0]) % nz, nz), lax.rem(me_x + (-key[1]) % nx, nx))

    barrier = pltpu.get_barrier_semaphore()
    for key, _ in others_list:
        pl.semaphore_signal(barrier, inc=1, device_id=owner(key), device_id_type=MESH)

    def whole(ref, sem):
        pltpu.make_async_copy(ref, ref, sem).wait()

    for k, (source, target) in enumerate([
            (coords_hbm, coords_ref), (live_hbm, live_ref), (out_hbm, out_ref)]):
        pltpu.make_async_copy(source, target, load_sem.at[k]).start()
    for k, source in enumerate((species_hbm, centers_hbm, others_hbm)):
        pltpu.make_async_copy(source, ints_ref.at[k], load_sem.at[3]).start()
    rows_in, rows_env, rows_up = in_hbm.shape[0], env_hbm.shape[0], up_hbm.shape[0]
    row = 0
    for source in (in_hbm, env_hbm, up_hbm):
        pltpu.make_async_copy(source, weights_ref.at[pl.ds(row, source.shape[0])], load_sem.at[4]).start()
        row += source.shape[0]
    whole(coords_ref, load_sem.at[0])
    whole(live_ref, load_sem.at[1])
    whole(ints_ref, load_sem.at[3])
    lane = lax.broadcasted_iota(jnp.int32, (1, n), 1)
    for a in range(bz):
        for b in range(bx):
            code = ints_ref[1, a, b : b + 1, :] + 128 * ints_ref[2, a, b : b + 1, :]
            code = jnp.where(lane < live_ref[a : a + 1, b : b + 1], code, -1)
            edges[mine, a, b : b + 1, :] = code.astype(F32)
            atoms[mine, a, b] = jnp.concatenate(
                [coords_ref[:, a, b, :], ints_ref[0, a, b : b + 1, :].astype(F32)], axis=0)
    pl.semaphore_wait(barrier, len(others_list))
    for key, s in others_list:
        for k, ref in enumerate((atoms, edges)):
            pltpu.make_async_remote_copy(
                src_ref=ref.at[mine], dst_ref=ref.at[s], send_sem=send_sem.at[k],
                recv_sem=recv_sem.at[k], device_id=user(key), device_id_type=MESH,
            ).start()

    whole(out_ref, load_sem.at[2])
    whole(weights_ref, load_sem.at[4])
    w_in = weights_ref[:rows_in]
    w_hi = rounded(w_in)
    w_lo = w_in - w_hi
    gap = jnp.zeros((nb, lat), F32)
    kin = 4 * nb + 4 * spec
    w_rows = [w_hi[:nb], w_hi[:nb], w_lo[:nb], gap, w_hi[nb:], w_lo[nb:]]
    if lat > kin:
        w_rows.append(jnp.zeros((lat - kin, lat), F32))
    in_t = jnp.concatenate(w_rows, axis=0).T.astype(BF16)[:, :kin]
    wr2 = jnp.concatenate(
        [jnp.concatenate([w_hi[:nb], w_hi[:nb]], axis=1), jnp.concatenate([w_lo[:nb], gap], axis=1)],
        axis=0).astype(BF16)
    env_t = weights_ref[rows_in : rows_in + rows_env]
    et_hi = rounded(env_t)
    et_lo = env_t - et_hi
    env_t2 = jnp.concatenate(
        [jnp.concatenate([et_hi, et_hi], axis=1), jnp.concatenate([et_lo, jnp.zeros_like(et_lo)], axis=1)],
        axis=0).astype(BF16)
    kpad = -(3 * ch) % lat
    env3 = jnp.concatenate(
        [et_hi, et_hi, et_lo] + ([jnp.zeros((kpad, lat), F32)] if kpad else []), axis=0
    ).T.astype(BF16)
    up = weights_ref[rows_in + rows_env :]
    up_hi = rounded(up)
    up_lo = up - up_hi
    up3 = jnp.concatenate([up_hi, up_hi, up_lo], axis=1).astype(BF16)
    up_t = jnp.concatenate(
        [x.T.astype(BF16) for x in (up_hi[:lat], up_hi[:lat], up_lo[:lat])]
        + [jnp.concatenate(
            [up_hi[lat:], up_hi[lat:], up_lo[lat:]]
            + ([jnp.zeros((kpad, lat), F32)] if kpad else []), axis=0).T.astype(BF16)],
        axis=1)
    out_col = jnp.broadcast_to(out_ref[...], (n, lat)).T

    rows_hot[...] = jnp.zeros_like(rows_hot)
    rows_hot_t[...] = jnp.zeros_like(rows_hot_t)
    grad[...] = jnp.zeros_like(grad)
    cz, cx = bz + 2, bx + 2
    total = cz * cx
    wide = cx * n
    inner = bx * n
    cells = [(a, b) for a in range(bz - 1, 2 * bz + 1) for b in range(bx - 1, 2 * bx + 1)]
    row_n = lax.broadcasted_iota(jnp.int32, (n, n), 0).astype(F32).astype(BF16)
    row_s = lax.broadcasted_iota(jnp.int32, (spec, n), 0).astype(F32)
    one, zero = jnp.ones((n, n), BF16), jnp.zeros((n, n), BF16)

    def place(a, b):
        return slots[((a // bz - 1) % nz, (b // bx - 1) % nx)], a % bz, b % bx

    def tables(rows):
        for a in rows:
            hl = {}
            for b in range(bx - 2, 2 * bx + 2):
                s, i, j = place(a, b)
                part = atoms[s, i, j]
                hi = rounded(part)
                hl[b] = jnp.concatenate([hi, part - hi], axis=0)
            for b in range(bx - 1, 2 * bx + 1):
                tab[a, b] = jnp.concatenate(
                    [hl[b - 1], hl[b], hl[b + 1], jnp.zeros((8, n), F32)], axis=0).astype(BF16)

    def decode(rows):
        c = slice(rows[0] * cx, (rows[-1] + 1) * cx)
        for i in range(rows[0] * cx, (rows[-1] + 1) * cx):
            s, y, x = place(*cells[i])
            codes[i : i + 1] = edges[s, y, x : x + 1, :]
        code = codes[c].astype(jnp.int32)
        o = code >> 7
        rows_c[c] = (code & 127).astype(F32)
        rows_o[c] = (o & 127).astype(F32)
        rows_p[c] = o >> 7
        rows_live[c] = (code >= 0).astype(F32)

    def gather(i):
        a, b = cells[i]
        p = rows_p[i : i + 1]
        hot_c = jnp.where(row_n == rows_c[i : i + 1].astype(BF16), one, zero)
        hot_o = jnp.where(row_n == rows_o[i : i + 1].astype(BF16), one, zero)
        both = jnp.concatenate([hot_c, hot_o], axis=1)
        hot[i] = both
        hot_t[i] = jnp.concatenate([hot_c.T, hot_o.T], axis=1)
        zr, xc = i // cx, i % cx
        if 1 <= zr <= bz and 1 <= xc <= bx:
            for dz in range(3):
                for dx in range(3):
                    col = dz * cx + xc - 1 + dx
                    masked = hot_o * (p == 3 * dz + dx).astype(F32).astype(BF16)
                    rows_hot[zr - 1, col * n : (col + 1) * n, (xc - 1) * n : xc * n] = masked
                    rows_hot_t[zr - 1, (xc - 1) * n : xc * n, col * n : (col + 1) * n] = masked.T
        around = jnp.concatenate([tab[a + dz, b] for dz in (-1, 0, 1)], axis=0)
        got = dot(around, both)
        at_c = got[40:48, :n]
        at_o = jnp.zeros((8, n), F32)
        for dz in range(3):
            for dx in range(3):
                at_o = jnp.where(p == 3 * dz + dx, got[32 * dz + 8 * dx : 32 * dz + 8 * dx + 8, n:], at_o)
        at_c = at_c[:4] + at_c[4:]
        at_o = at_o[:4] + at_o[4:]
        diffs[i] = at_o - at_c
        xs[:, i * n : (i + 1) * n] = jnp.concatenate(
            [(row_s == at_c[3:4]).astype(F32), (row_s == at_o[3:4]).astype(F32)], axis=0).astype(BF16)

    def geometry(rows):
        c = slice(rows[0] * cx, (rows[-1] + 1) * cx)
        p = rows_p[c]
        third = (p >= 3).astype(jnp.int32) + (p >= 6).astype(jnp.int32)
        r = [
            diffs[c, 0, :] + (third - 1).astype(F32),
            diffs[c, 1, :] + (p - 3 * third - 1).astype(F32),
            diffs[c, 2, :],
        ]
        dist = jnp.sqrt(r[0] * r[0] + r[1] * r[1] + r[2] * r[2] + SOFTEN)
        inv = 1.0 / dist
        q = dist / CUTOFF
        rest = 1.0 - q * q
        envelope = rest * rest
        scale = inv * envelope
        t1 = math.pi * (q - 0.5)
        t2 = t1 * t1
        s1, c1 = jnp.ones_like(q), jnp.ones_like(q)
        for m in range(7, 0, -1):
            s1 = 1.0 - t2 * s1 * (1.0 / ((2 * m - 1) * (2 * m)))
            c1 = 1.0 - t2 * c1 * (1.0 / ((2 * m) * (2 * m + 1)))
        c1 = -t1 * c1
        s0, c0, sk, ck = jnp.zeros_like(s1), jnp.ones_like(c1), s1, c1
        for k in range(nb):
            sins[k, c] = sk
            coss[k, c] = ck
            rad[k, c] = sk * scale
            s0, sk = sk, 2.0 * c1 * sk - s0
            c0, ck = ck, 2.0 * c1 * ck - c0
        for m in range(3):
            harm[m, c] = r[m] * inv
            geo[m, c] = r[m]
        env_grad[c] = jnp.zeros_like(q)
        geo[3, c] = envelope
        geo[4, c] = inv
        geo[5, c] = (-4.0 / CUTOFF) * q * rest

    def ids_of(zr):
        return list(range(zr * cx, (zr + 1) * cx))

    def inner_of(zr):
        return ids_of(zr)[1:-1]

    def latents(rows):
        pres, lows, mls = {}, {}, {}
        for zr in rows:
            span = slice(zr * wide, (zr + 1) * wide)
            radial = join([rad[:, i, :] for i in ids_of(zr)], 1)
            rh = rounded(radial)
            x_s = xs[:, span]
            pres[zr] = dot(in_t, jnp.concatenate([
                jnp.concatenate([rh, radial - rh], axis=0).astype(BF16),
                jnp.concatenate([rh, jnp.zeros_like(rh)], axis=0).astype(BF16), x_s, x_s], axis=0))
        for zr in rows:
            span = slice(zr * wide, (zr + 1) * wide)
            pre = pres[zr]
            sig = 0.5 + 0.5 * jnp.tanh(0.5 * pre)
            latent = pre * sig
            sigs[:, span] = sig
            lats[:, span] = latent
            lh, ll = split(latent)
            if 1 <= zr <= bz:
                l2[zr - 1, 0] = lh[:, n : n + inner]
                l2[zr - 1, 1] = ll[:, n : n + inner]
            lows[zr] = dot(env_t2, jnp.concatenate([lh, ll], axis=0))
        for zr in rows:
            span = slice(zr * wide, (zr + 1) * wide)
            ids = ids_of(zr)
            w = lows[zr]
            w = (w[:ch] + w[ch:]) * join([rows_live[i : i + 1] for i in ids], 1)
            wts[:, span] = w
            msgs = jnp.concatenate(
                [w] + [w * join([harm[m, i : i + 1] for i in ids], 1) for m in range(3)], axis=0)
            mls[zr] = split(msgs)
            mh, ml = mls[zr]
            for t, i in enumerate(ids):
                cut = slice(t * n, (t + 1) * n)
                hot_c = hot_t[i, :, :n]
                feat[:, i * n : (i + 1) * n] = dot(
                    jnp.concatenate([mh[:, cut], ml[:, cut]], axis=1),
                    jnp.concatenate([hot_c, hot_c], axis=0)).astype(BF16)

    early, late = list(range(2, cz)), [0, 1]
    for k, ref in enumerate((atoms, edges)):
        received = ref.at[pl.ds(0, len(others_list))]
        whole(received, recv_sem.at[k])
        whole(received, send_sem.at[k])
    every = list(range(cz))
    decode(every)
    tables(range(bz - 2, 2 * bz + 2))
    for i in range(total):
        gather(i)
    geometry(every)
    latents(every)

    row_16 = lax.broadcasted_iota(jnp.int32, (16, n), 0)
    out_rows = jnp.concatenate([out_col] * bx, axis=1)
    inner_rows = range(1, bz + 1)
    f_cs, f_os, us, joins, raws = {}, {}, {}, {}, {}
    for zr in inner_rows:
        f_cs[zr] = join([dot(feat[:, i * n : (i + 1) * n], hot[i, :, :n]) for i in inner_of(zr)], 1)
        f_os[zr] = dot(feat[:, (zr - 1) * wide : (zr + 2) * wide], rows_hot[zr - 1])
    for zr in inner_rows:
        prod4 = f_cs[zr] * f_os[zr]
        prod = prod4[:ch] + prod4[ch : 2 * ch] + prod4[2 * ch : 3 * ch] + prod4[3 * ch :]
        ph, pl_ = split(prod)
        parts = [l2[zr - 1, 0], l2[zr - 1, 1], l2[zr - 1, 0], ph, pl_, ph]
        if kpad:
            parts.append(jnp.zeros((kpad, inner), BF16))
        us[zr] = dot(up_t, jnp.concatenate(parts, axis=0))
    for zr in inner_rows:
        env_row = join([geo[3, i : i + 1] for i in inner_of(zr)], 1)
        alive = join([rows_live[i : i + 1] for i in inner_of(zr)], 1)
        u = us[zr]
        sig = 0.5 + 0.5 * jnp.tanh(0.5 * u)
        hid = u * sig
        raws[zr] = jnp.sum(out_rows * hid, axis=0, keepdims=True) * alive
        d_u = out_rows * (alive * env_row) * (sig + hid * (1.0 - sig))
        dh, dl = split(d_u)
        joins[zr] = dot(up3, jnp.concatenate([dh, dl, dh], axis=0))
    dcs, dos = {}, {}
    for zr in inner_rows:
        d_join = joins[zr]
        dlat_own[zr - 1] = d_join[:lat]
        d_prod = jnp.concatenate([d_join[lat:]] * 4, axis=0)
        dcs[zr] = split(d_prod * f_os[zr])
        dos[zr] = jnp.concatenate(split(d_prod * f_cs[zr]), axis=1)

    def feature_gradient(rows):
        for r in rows:
            acc = None
            for zr in inner_rows:
                if abs(r - zr) <= 1:
                    at = r - zr + 1
                    block = rows_hot_t[zr - 1, :, at * wide : (at + 1) * wide]
                    term = dot(dos[zr], jnp.concatenate([block, block], axis=0))
                    acc = term if acc is None else acc + term
            if r in inner_rows:
                side = jnp.zeros((4 * ch, n), F32)
                tops = [side]
                for t, i in enumerate(inner_of(r)):
                    cut = slice(t * n, (t + 1) * n)
                    raw = raws[r][:, cut]
                    env_grad[i : i + 1] = raw
                    e_row = raw * geo[3, i : i + 1]
                    e_hi = rounded(e_row)
                    e_lo = jnp.where(row_16 == 0, e_row - e_hi, 0.0).astype(BF16)
                    e_hi = jnp.where(row_16 == 0, e_hi, 0.0).astype(BF16)
                    hot_c = hot_t[i, :, :n]
                    dch, dcl = dcs[r]
                    both = dot(
                        jnp.concatenate([
                            jnp.concatenate([dch[:, cut], e_hi], axis=0),
                            jnp.concatenate([dcl[:, cut], e_lo], axis=0)], axis=1),
                        jnp.concatenate([hot_c, hot_c], axis=0))
                    tops.append(both[: 4 * ch])
                    grad[centre, r - 1, t, 3:4] = -both[4 * ch : 4 * ch + 1]
                acc = acc + jnp.concatenate(tops + [side], axis=1)
            dfeat[:, r * wide : (r + 1) * wide] = acc

    def backward(rows):
        dms, dls = {}, {}
        for zr in rows:
            dm = []
            for i in ids_of(zr):
                hot_c = hot[i, :, :n]
                fh, fl = split(dfeat[:, i * n : (i + 1) * n])
                dm.append(dot(jnp.concatenate([fh, fl], axis=1), jnp.concatenate([hot_c, hot_c], axis=0)))
            dms[zr] = join(dm, 1)
        for zr in rows:
            ids = ids_of(zr)
            dm = dms[zr]
            dw = dm[:ch]
            for m in range(3):
                dw = dw + dm[(m + 1) * ch : (m + 2) * ch] * join([harm[m, i : i + 1] for i in ids], 1)
            dw = dw * join([rows_live[i : i + 1] for i in ids], 1)
            wh, wl = split(dw)
            parts = [wh, wl, wh]
            if kpad:
                parts.append(jnp.zeros((kpad, wide), BF16))
            dls[zr] = dot(env3, jnp.concatenate(parts, axis=0))
        for zr in rows:
            span = slice(zr * wide, (zr + 1) * wide)
            d_lat = dls[zr]
            if 1 <= zr <= bz:
                side = jnp.zeros((lat, n), F32)
                d_lat = d_lat + jnp.concatenate([side, dlat_own[zr - 1], side], axis=1)
            sig = sigs[:, span]
            dh, dl = split(d_lat * (sig + lats[:, span] * (1.0 - sig)))
            d_r = dot(wr2, jnp.concatenate([dh, dl], axis=0))
            d_r = d_r[:nb] + d_r[nb:]
            for t, i in enumerate(ids_of(zr)):
                drad[:, i, :] = d_r[:, t * n : (t + 1) * n]
        for zr in rows:
            span = slice(zr * wide, (zr + 1) * wide)
            w = wts[:, span]
            for m in range(3):
                d_h = jnp.sum(dms[zr][(m + 1) * ch : (m + 2) * ch] * w, axis=0, keepdims=True)
                for t, i in enumerate(ids_of(zr)):
                    dharm[m, i : i + 1] = d_h[:, t * n : (t + 1) * n]

    def radial_backward(rows):
        c = slice(rows[0] * cx, (rows[-1] + 1) * cx)
        sum_s = drad[0, c] * sins[0, c]
        sum_c = drad[0, c] * coss[0, c]
        for k in range(1, nb):
            sum_s = sum_s + drad[k, c] * sins[k, c]
            sum_c = sum_c + (k + 1.0) * (drad[k, c] * coss[k, c])
        inv, env_slope = geo[4, c], geo[5, c]
        scale = inv * geo[3, c]
        d_dist = (
            (math.pi / CUTOFF) * sum_c * scale
            - sum_s * scale * inv
            + (sum_s * inv + env_grad[c]) * env_slope
        )
        for m in range(3):
            d_dist = d_dist - dharm[m, c] * geo[m, c] * (inv * inv)
        for m in range(3):
            d_m = d_dist * harm[m, c] + dharm[m, c] * inv
            hi = rounded(d_m)
            gr[c, m, :] = hi
            gr[c, m + 4, :] = d_m - hi
        gr[c, 3, :] = jnp.zeros_like(inv)
        gr[c, 7, :] = jnp.zeros_like(inv)

    def scatter(i):
        a, b = cells[i]
        g8 = gr[i]
        p = rows_p[i : i + 1]
        stack = [g8] + [jnp.where(p == off, g8, 0.0) for off in range(9)]
        out = dot(jnp.concatenate(stack, axis=0).astype(BF16), hot_t[i])
        s, y, x = place(a, b)
        grad[s, y, x] -= out[:8, :n]
        for off in range(9):
            s, y, x = place(a + off // 3 - 1, b + off % 3 - 1)
            grad[s, y, x] += out[8 + 8 * off : 16 + 8 * off, n:]

    second = {}

    def give(later):
        for key, s in others_list:
            if s in second or s in later:
                continue
            i = index[s]
            for y in range(bz):
                for x in range(bx):
                    acc = grad[s, y, x]
                    give_ref[i, y, x] = acc[:4] + acc[4:]
            second[s] = pltpu.make_async_remote_copy(
                src_ref=give_ref.at[i], dst_ref=back.at[i], send_sem=send_sem.at[2],
                recv_sem=recv_sem.at[2], device_id=owner(key), device_id_type=MESH,
            )
            second[s].start()

    def targets(rows):
        return {
            place(cells[i][0] + dz, cells[i][1] + dx)[0]
            for zr in rows for i in ids_of(zr) for dz in (-1, 0, 1) for dx in (-1, 0, 1)}

    feature_gradient(early)
    backward(early[::-1])
    radial_backward(early)
    for zr in reversed(early):
        for i in ids_of(zr):
            scatter(i)
    give(targets(late))
    feature_gradient(late)
    backward(late[::-1])
    radial_backward(late)
    for zr in reversed(late):
        for i in ids_of(zr):
            scatter(i)
    give(set())
    whole(give_ref, send_sem.at[2])
    whole(back, recv_sem.at[2])
    for a in range(bz):
        for b in range(bx):
            acc = grad[mine, a, b]
            acc = acc[:4] + acc[4:]
            for s in range(len(others_list)):
                acc = acc + back[s, a, b]
            result_ref[:, a, b, :] = -acc


def deliver(result_ref, energy_ref, force_ref, sem):
    copies = [
        pltpu.make_async_copy(result_ref.at[3], energy_ref, sem.at[0]),
        pltpu.make_async_copy(result_ref.at[pl.ds(0, 3)], force_ref, sem.at[1]),
    ]
    for copy in copies:
        copy.start()
    for copy in copies:
        copy.wait()


def solution(mesh):
    nz, nx = mesh.shape["gz"], mesh.shape["xy"]

    def body(coords, species, centers, others, live_count, in_weight, env_weight, up_weight, out_weight):
        _, bz, bx, n = coords.shape
        lat, ch = env_weight.shape
        nb = 8
        spec = (in_weight.shape[0] - nb) // 2
        cells = (bz + 2) * (bx + 2)
        ns = len(neighbours(nz, nx)) - 1
        vmem = lambda shape, dtype=F32: pltpu.VMEM(shape, dtype)
        args = (coords, species, centers, others, live_count, in_weight, env_weight.T, up_weight,
                out_weight[None])
        scratch = [
            vmem(coords.shape),
            vmem((3, bz, bx, n), jnp.int32),
            vmem((bz, bx), jnp.int32),
            vmem((sum(w.shape[0] for w in args[5:8]), lat)),
            vmem((1, lat)),
            vmem((ns + 1, bz, bx, 4, n)),
            vmem((ns + 1, bz, bx, n)),
            vmem((3 * bz, 3 * bx, 32, n), BF16),
            vmem((cells, n, 2 * n), BF16),
            vmem((cells, n, 2 * n), BF16),
            vmem((bz, 3 * (bx + 2) * n, bx * n), BF16),
            vmem((bz, bx * n, 3 * (bx + 2) * n), BF16),
            vmem((cells, n)),
            vmem((cells, n)),
            vmem((cells, n)),
            vmem((cells, n), jnp.int32),
            vmem((cells, n)),
            vmem((cells, 4, n)),
            vmem((6, cells, n)),
            vmem((2 * spec, cells * n), BF16),
            vmem((nb, cells, n)),
            vmem((nb, cells, n)),
            vmem((nb, cells, n)),
            vmem((3, cells, n)),
            vmem((bz, 2, lat, bx * n), BF16),
            vmem((lat, cells * n)),
            vmem((lat, cells * n)),
            vmem((ch, cells * n)),
            vmem((4 * ch, cells * n), BF16),
            vmem((4 * ch, cells * n)),
            vmem((bz, lat, bx * n)),
            vmem((cells, n)),
            vmem((3, cells, n)),
            vmem((nb, cells, n)),
            vmem((cells, 8, n)),
            vmem((ns + 1, bz, bx, 8, n)),
            vmem((ns, bz, bx, 4, n)),
            vmem((ns, bz, bx, 4, n)),
            pltpu.SemaphoreType.DMA((3,)),
            pltpu.SemaphoreType.DMA((3,)),
            pltpu.SemaphoreType.DMA((5,)),
        ]
        specs = [pl.BlockSpec(memory_space=pl.ANY) for _ in args]
        result = pl.pallas_call(
            functools.partial(kernel, nz, nx, bz, bx, nb, spec, ch, lat),
            out_shape=pltpu.VMEM((4, bz, bx, n), F32),
            in_specs=specs,
            out_specs=pl.BlockSpec(memory_space=pltpu.VMEM),
            scratch_shapes=scratch,
            compiler_params=pltpu.CompilerParams(collective_id=0, has_side_effects=True),
        )(*args)
        return pl.pallas_call(
            deliver,
            out_shape=(jax.ShapeDtypeStruct((bz, bx, n), F32), jax.ShapeDtypeStruct((3, bz, bx, n), F32)),
            in_specs=[pl.BlockSpec(memory_space=pltpu.VMEM)],
            out_specs=(pl.BlockSpec(memory_space=pl.ANY), pl.BlockSpec(memory_space=pl.ANY)),
            scratch_shapes=[pltpu.SemaphoreType.DMA((2,))],
        )(pltpu.with_memory_space_constraint(result, pltpu.VMEM))

    in_specs = (
        P(None, "gz", "xy", None), P("gz", "xy", None), P("gz", "xy", None), P("gz", "xy", None),
        P("gz", "xy"), P(), P(), P(), P(),
    )
    out_specs = (P("gz", "xy", None), P(None, "gz", "xy", None))
    return jax.shard_map(body, mesh=mesh, in_specs=in_specs, out_specs=out_specs, check_vma=False)
```
